32 devices in a mesh: fsdp: 8 (over z, x), grp: 4 (over y, core).
Axes of the slice: x: 2, y: 2, z: 4, core: 2. Of those that a mesh axis runs over, the one named last changes fastest.
Arguments:
- gradient: bfloat16 [24, 512, 512], P('fsdp', 'grp'), may hold values from -6 to 6
- left_factor: bfloat16 [96, 512, 512], P(('fsdp', 'grp'))
- right_factor: bfloat16 [96, 512, 512], P(('fsdp', 'grp'))
- block_owner: int32 [24], replicated, may hold values from 0 to 31, as said below
Outputs:
- preconditioned: bfloat16 [24, 512, 512], P('fsdp', 'grp')
The draws below stay inside these ranges and needn't reach their ends.
Inputs may be any that keep to these rules, and one draw needn't show every extreme that they name: block_owner[b] is a device index, fsdp index times 4 plus grp index. The 3 blocks homed at one fsdp index go to devices of 3 different fsdp indices; the devices of each fsdp index own 3 blocks in all; no device owns more than 3 blocks, and at every fsdp index one device owns exactly 3.
All inputs are finite; a program needn't handle non-finite values.
Results may differ from the reference program's by a relative error of at most 0.0049.
Values may be sent and summed in bfloat16 or wider, within the bound.
A program may use at most 64 MiB of HBM per device.

```python
import jax
import jax.numpy as jnp
from jax import lax

B = 512
CAP = 3
BLOCKS_COL = 3
BLOCKS = 24
N_FSDP = 8
N_GRP = 4


def draw_factor_common(key, salt_value):
    key_diag, key_noise = jax.random.split(jax.random.fold_in(key, salt_value))
    count = N_FSDP * N_GRP * CAP
    diagonal = jax.random.uniform(key_diag, (count, B), jnp.float32, 0.5, 1.5)
    noise = jax.random.normal(key_noise, (count, B, B), jnp.float32) * (0.5 / B ** 0.5)
    identity = jnp.eye(B, dtype=jnp.float32)
    return noise + diagonal[:, :, None] * identity[None, :, :]


def draw_left_factor(key, part):
    return draw_factor_common(key, 21).astype(jnp.bfloat16)


def draw_right_factor(key, part):
    return draw_factor_common(key, 37).astype(jnp.bfloat16)


def draw_block_owner(key, part):
    key_offsets, key_full, key_order = jax.random.split(jax.random.fold_in(key, 11), 3)
    offsets = jax.random.permutation(key_offsets, N_FSDP)[:BLOCKS_COL].astype(jnp.int32)
    halfway = N_FSDP // 2
    has_half = jnp.any(offsets == halfway)
    offsets = offsets.at[0].set(jnp.where(has_half, offsets[0], halfway)).astype(jnp.int32)
    column_ids = jnp.arange(N_FSDP, dtype=jnp.int32)
    dest_column = (column_ids[:, None] + offsets[None, :]) % N_FSDP
    source_column = (column_ids[:, None] - offsets[None, :]) % N_FSDP
    arrival_rank = jnp.sum(source_column[:, None, :] < source_column[:, :, None], axis=2).astype(jnp.int32)
    full_owner = jax.random.randint(key_full, (N_FSDP,), 0, N_GRP)
    spare_slots = N_GRP * CAP - CAP
    priority = jax.random.randint(key_order, (N_FSDP, spare_slots), 0, 1 << 20) * spare_slots + jnp.arange(spare_slots, dtype=jnp.int32)[None, :]
    spare_order = jnp.argsort(priority, axis=1).astype(jnp.int32)
    later_owner = jnp.take_along_axis(spare_order, jnp.clip(arrival_rank - CAP, 0, spare_slots - 1), axis=1) // CAP
    later_owner = later_owner + (later_owner >= full_owner[:, None]).astype(jnp.int32)
    owner_group = jnp.where(arrival_rank < CAP, full_owner[:, None], later_owner)
    picked = owner_group[dest_column, jnp.arange(BLOCKS_COL, dtype=jnp.int32)[None, :]]
    return (dest_column * N_GRP + picked).reshape(-1).astype(jnp.int32)


def shard_levels(rng, shape, cuts, low, top_value):
    def one(axis_at, shards_of):
        heights = jax.random.uniform(jax.random.fold_in(jax.random.fold_in(rng, 6), axis_at), (shards_of,), jnp.float32, low / len(cuts), top_value / len(cuts))
        return jnp.repeat(jnp.exp(heights), shape[axis_at] // shards_of).reshape((-1,) + (1,) * (len(shape) - axis_at - 1))

    level = one(*cuts[0])
    for cut in cuts[1:]:
        level = level * one(*cut)
    return level


def bell_draw(own_key, extent, spread, limit, cuts=(), held_as=jnp.bfloat16):
    entries = jax.random.normal(own_key, extent, jnp.float32) * spread
    if len(cuts) > 0:
        entries = shard_levels(own_key, extent, cuts, -0.22, 0.18) * entries
    return jnp.clip(entries, min=-limit, max=limit).astype(held_as)


def setup_inputs(seed: int = 0) -> dict:
    streams_of = jax.random.split(jax.random.key(seed), 5)
    return {
        "gradient": bell_draw(streams_of[0], (BLOCKS, B, B), 1.0, 6.0, ((0, 8), (1, 4))),
        "left_factor": draw_left_factor(jax.random.fold_in(streams_of[4], 71), 0),
        "right_factor": draw_right_factor(jax.random.fold_in(streams_of[4], 71), 0),
        "block_owner": draw_block_owner(jax.random.fold_in(streams_of[4], 71), 0),
    }


def reference(gradient, left_factor, right_factor, block_owner):
    block_ids = jnp.arange(BLOCKS, dtype=jnp.int32)
    earlier = (block_owner[None, :] == block_owner[:, None]) & (block_ids[None, :] < block_ids[:, None])
    slot_index = (block_owner + 0).astype(jnp.int32) * CAP + jnp.sum(earlier, axis=1).astype(jnp.int32)

    def precondition_group(packed):
        grad_group, indices = packed
        left_group = jnp.take(left_factor, indices, axis=0).astype(jnp.float32)
        right_group = jnp.take(right_factor, indices, axis=0).astype(jnp.float32)
        product = jnp.einsum("kab,kbc->kac", left_group, grad_group.astype(jnp.float32)).astype(jnp.bfloat16)
        return jnp.einsum("kab,kbc->kac", product.astype(jnp.float32), right_group).astype(jnp.bfloat16)

    grouped = gradient.reshape(BLOCKS // BLOCKS_COL, BLOCKS_COL, B, B)
    indices_grouped = slot_index.reshape(BLOCKS // BLOCKS_COL, BLOCKS_COL).astype(jnp.int32)
    stacked = lax.map(precondition_group, (grouped, indices_grouped))
    return stacked.reshape(BLOCKS, B, B)
```

```python
import functools

import jax
import jax.numpy as jnp
from jax import lax
from jax.experimental import pallas as pl
from jax.experimental.pallas import tpu as pltpu
from jax.sharding import PartitionSpec as P

MESH = pl.DeviceIdType.MESH
CHUNKS = 4
TEAMS = (('G', 'far', 'near'), ('F', 'far'), ('F', 'far'))
GRADIENT_STEPS = ("I0", "I1", "I2", "I3", "I4", "I5", "R", "H", "O0", "O1", "O2", "O3")
WHEN = {
    ('I0', 0): (0, 1, 2, 3),
    ('S0', 1): (4, 5, 6, 7, 8, 9, 10, 13),
    ('H', 1): (11, 12, 14, 15, 16, 17, 19, 22),
    ('G0', 1): (18, 20, 21, 23),
    ('S0', 2): (24, 25, 27, 28, 29, 30, 35, 43),
    ('I1', 0): (26, 33, 40, 51),
    ('H', 2): (31, 34, 36, 37, 39, 41, 46, 52),
    ('O0', 1): (32, 38, 44, 48, 54, 55, 60, 68),
    ('I2', 0): (42, 53, 58, 65),
    ('G0', 2): (45, 47, 49, 50),
    ('I3', 0): (56, 62, 70, 77),
    ('G1', 1): (57, 63, 66, 71),
    ('O1', 1): (59, 64, 72, 78, 83, 87, 94, 99),
    ('G2', 1): (61, 67, 69, 74),
    ('O0', 2): (73, 76, 79, 81, 82, 86, 90, 101),
    ('O2', 1): (75, 80, 85, 92, 98, 106, 111, 120),
    ('O3', 1): (84, 88, 97, 109, 119, 123, 129, 138),
    ('G1', 2): (89, 91, 95, 100),
    ('G2', 2): (93, 96, 102, 104),
    ('O1', 2): (103, 107, 112, 118, 121, 125, 128, 133),
    ('I4', 0): (105, 108, 113, 115),
    ('I5', 0): (110, 114, 117, 122),
    ('LG', 1): (116,),
    ('R', 0): (124, 127, 131, 142),
    ('O2', 2): (126, 130, 135, 141, 145, 150, 152, 156),
    ('H', 0): (132, 136, 139, 151),
    ('O4', 1): (134, 137, 147, 159),
    ('O5', 1): (140, 144, 154, 162),
    ('O3', 2): (143, 146, 149, 155, 160, 163, 166, 169),
    ('O0', 0): (148, 153, 158, 164),
    ('LG', 2): (157,),
    ('O1', 0): (161, 165, 167, 172),
    ('O2', 0): (168, 171, 175, 181),
    ('O4', 2): (170, 173, 176, 178),
    ('O5', 2): (174, 177, 179, 182),
    ('O3', 0): (180, 183, 184, 185),
}


def per_device(gradient, left_factor, right_factor, block_owner):
    local_blocks = gradient.shape[0]
    piece_rows = gradient.shape[1]
    block_width = gradient.shape[2]
    slot_count = left_factor.shape[0]
    columns = lax.axis_size("fsdp")
    groups = lax.axis_size("grp")
    column = lax.axis_index("fsdp")
    owners_all = block_owner.reshape(columns, local_blocks)
    dest_column = owners_all // groups
    dest_group = owners_all % groups
    mine_column = lax.dynamic_index_in_dim(dest_column, column, 0, keepdims=False)
    column_ids = jnp.arange(columns, dtype=jnp.int32)
    matching = mine_column[None, :] == column_ids[:, None]
    pick_send = matching.astype(jnp.bfloat16)
    outgoing = jnp.einsum(
        "cj,jrd->crd", pick_send, gradient, preferred_element_type=jnp.float32
    ).astype(jnp.bfloat16)
    arrived = lax.all_to_all(
        outgoing.reshape(columns * piece_rows, block_width),
        "fsdp",
        split_axis=0,
        concat_axis=0,
        tiled=True,
    )
    arrived = arrived.reshape(columns, piece_rows, block_width)
    toward = dest_column == column
    live_source = jnp.sum(toward.astype(jnp.int32), axis=1) > 0
    target = jnp.sum(jnp.where(toward, dest_group, 0), axis=1)
    same_owner = (target[None, :] == target[:, None]) & live_source[None, :] & live_source[:, None]
    before = column_ids[None, :] < column_ids[:, None]
    rank_slot = jnp.sum((same_owner & before).astype(jnp.int32), axis=1)
    group_ids = jnp.arange(groups, dtype=jnp.int32)
    slot_ids = jnp.arange(slot_count, dtype=jnp.int32)
    routing = (
        live_source[None, None, :]
        & (target[None, None, :] == group_ids[:, None, None])
        & (rank_slot[None, None, :] == slot_ids[None, :, None])
    )
    routing = routing.astype(jnp.bfloat16)
    packed = jnp.einsum(
        "oks,srd->kord", routing, arrived, preferred_element_type=jnp.float32
    ).astype(jnp.bfloat16)
    packed = packed.reshape(slot_count, groups * piece_rows, block_width)
    blocks = lax.all_to_all(packed, "grp", split_axis=1, concat_axis=1, tiled=True)
    left_product = jnp.einsum(
        "kab,kbc->kac", left_factor, blocks, preferred_element_type=jnp.float32
    ).astype(jnp.bfloat16)
    result = jnp.einsum(
        "kab,kbc->kac", left_product, right_factor, preferred_element_type=jnp.float32
    ).astype(jnp.bfloat16)
    returned = lax.all_to_all(result, "grp", split_axis=1, concat_axis=1, tiled=True)
    returned = returned.reshape(slot_count, groups, piece_rows, block_width)
    unpacked = jnp.einsum(
        "oks,kord->srd", routing, returned, preferred_element_type=jnp.float32
    ).astype(jnp.bfloat16)
    homeward = lax.all_to_all(
        unpacked.reshape(columns * piece_rows, block_width),
        "fsdp",
        split_axis=0,
        concat_axis=0,
        tiled=True,
    )
    homeward = homeward.reshape(columns, piece_rows, block_width)
    return jnp.einsum(
        "cj,crd->jrd", pick_send, homeward, preferred_element_type=jnp.float32
    ).astype(jnp.bfloat16)


def stages_of(team, chunks):
    if team[0] == "G":
        return [(name, chunks) for name in GRADIENT_STEPS]
    found = [(name, chunks) for name in ("G0", "G1", "G2")]
    found += [(name, 2 * chunks) for name in ("S0", "H", "O0", "O1", "O2", "O3")]
    return found + [("LG", 1), ("O4", chunks), ("O5", chunks)]


def timetable(teams, chunks):
    steps = []
    for t, team in enumerate(teams):
        for name, count in stages_of(team, chunks):
            first = chunks if name in ("O4", "O5") else 0
            for i in range(count):
                steps.append((WHEN[(name, t)][i], len(steps), name, t, first + i))
    return [step[2:] for step in sorted(steps)]


def scratch_of(teams, chunks, blocks, columns, groups, rows, width, dtype):
    w = width // chunks
    vmem = lambda *shape: pltpu.VMEM(shape, dtype)
    dma = pltpu.SemaphoreType.DMA
    held = {
        "gv": vmem(blocks, rows, width),
        "lv": vmem(blocks, width, width),
        "rv": vmem(blocks, width, width),
        "load": dma((3,)),
        "power": pltpu.SMEM((columns,), jnp.int32),
    }

    def copies(key, count):
        held[key + ("snd",)] = dma((count,))
        held[key + ("rcv",)] = dma((count,))

    def route(key, count):
        for k in range(count):
            held[("cand",) + key + (k,)] = vmem(4, rows, w)
            held[("last",) + key + (k,)] = vmem(rows, w)
            held[("sel",) + key + (k,)] = vmem(rows, w)
        for name in ("f", "b", "bf", "l"):
            copies((name,) + key, count)

    def gather(key, count):
        for k in range(count):
            held[("all",) + key + (k,)] = vmem(groups, rows, w)
        for name in ("across", "mate0", "mate1"):
            copies((name,) + key, count)

    def scatter(key, count):
        for k in range(count):
            held[("pc",) + key + (k,)] = vmem(2, 2, rows, w)
            held[("rcvc",) + key + (k,)] = vmem(2, rows, w)
            held[("sely",) + key + (k,)] = vmem(rows, w)
            held[("rcvy",) + key + (k,)] = vmem(rows, w)
        for name in ("home", "back"):
            copies((name,) + key, count)

    for t, team in enumerate(teams):
        held[("fin", t)] = vmem(rows, width)
        if team[0] == "G":
            route((t, "I"), chunks)
            gather((t, "I"), chunks)
            held[("lp", t)] = vmem(width, width)
            scatter((t, "O"), chunks)
            route((t, "O"), chunks)
        else:
            gather((t, "I"), chunks)
            scatter((t, "O"), 2 * chunks)
            route((t, "O"), 2 * chunks)
            gather((t, "O"), chunks)
            held[("lrow", t)] = vmem(rows, width)
            held[("lg", t)] = vmem(rows, width)
    return held


def preconditioner_kernel(
    teams, chunks, names, columns, groups, blocks, rows, width,
    owner_ref, g_hbm, l_hbm, r_hbm, out_ref, *rest,
):
    ref = dict(zip(names, rest))
    col = lax.axis_index("fsdp")
    grp = lax.axis_index("grp")
    core = grp % 2
    half = grp // 2
    mate = half * 2 + (1 - core)
    across = (1 - half) * 2 + core
    diagonal = (1 - half) * 2 + (1 - core)
    w = width // chunks
    zero = jnp.int32(0)

    def cols_of(q):
        return slice(q * w, (q + 1) * w)

    def partner(s):
        d, b = 0, 1
        while b < columns:
            v = (col // b) % 2
            d, b = d + b * ((1 - v) if s & b else v), 2 * b
        return d

    gv, lv, rv = ref["gv"], ref["lv"], ref["rv"]
    loads = [
        pltpu.make_async_copy(g_hbm, gv, ref["load"].at[0]),
        pltpu.make_async_copy(l_hbm, lv, ref["load"].at[1]),
        pltpu.make_async_copy(r_hbm, rv, ref["load"].at[2]),
    ]
    for load in loads:
        load.start()

    far, near = columns // 2, columns // 4
    barrier = pltpu.get_barrier_semaphore()
    for s in (1, near, far):
        pl.semaphore_signal(barrier, inc=1, device_id={"fsdp": partner(s)}, device_id_type=MESH)
    for g in (mate, across):
        pl.semaphore_signal(barrier, inc=1, device_id={"grp": g}, device_id_type=MESH)

    def look_up(table, index):
        found = zero
        for n, value in enumerate(table):
            found = jnp.where(index == n, value, found)
        return found

    power = ref["power"]
    for d in range(columns):
        power[d] = jnp.int32(2 ** d)
    to = [[owner_ref[c * blocks + j] // groups for j in range(blocks)] for c in range(columns)]
    left_over = [[(jnp.int32(j), to[c][j], power[to[c][j]]) for j in range(blocks)] for c in range(columns)]
    pick, dest = [], []
    full = 2 ** columns - 1
    while len(left_over[0]) > 1:
        m = len(left_over[0])
        count = m ** columns
        tall = -(-count // 1024) * 8
        inverse = -(-(2 ** 17) // m)
        index = (
            lax.broadcasted_iota(jnp.int32, (tall, 128), 0) * 128
            + lax.broadcasted_iota(jnp.int32, (tall, 128), 1)
        )
        rest_of, reach = index, jnp.zeros((tall, 128), jnp.int32)
        for c in range(columns):
            upper = (rest_of * inverse) >> 17
            digit = rest_of - upper * m
            bit = jnp.full((tall, 128), left_over[c][m - 1][2], jnp.int32)
            for i in range(m - 1):
                bit = jnp.where(digit == i, left_over[c][i][2], bit)
            reach, rest_of = reach | bit, upper
        chosen = jnp.min(jnp.where((reach == full) & (index < count), index, count - 1))
        pick_t, dest_t = [], []
        for c in range(columns):
            upper = (chosen * inverse) >> 17
            digit, chosen = chosen - upper * m, upper
            pick_t.append(look_up([e[0] for e in left_over[c]], digit))
            dest_t.append(look_up([e[1] for e in left_over[c]], digit))
            left_over[c] = [
                tuple(jnp.where(digit <= i, b, a) for a, b in zip(left_over[c][i], left_over[c][i + 1]))
                for i in range(m - 1)
            ]
        pick.append(pick_t)
        dest.append(dest_t)
    pick.append([left_over[c][0][0] for c in range(columns)])
    dest.append([left_over[c][0][1] for c in range(columns)])

    owner_group = zero
    for c in range(columns):
        for j in range(blocks):
            owner_group = jnp.where(to[c][j] == col, owner_ref[c * blocks + j] % groups, owner_group)
    owner_core = owner_group % 2
    owner_half = owner_group // 2
    reaches = []
    for c in range(columns):
        hit = zero
        for j in range(blocks):
            hit = jnp.where(to[c][j] == col, 1, hit)
        reaches.append(hit)

    def source_of(t, d):
        found = zero
        for c in range(columns):
            found = jnp.where(dest[t][c] == d, c, found)
        return found

    def place_among(wanted, f, other):
        found = jnp.int32(other)
        for n, s in enumerate((0, 1, f, f + 1)):
            found = jnp.where(wanted == partner(s), n, found)
        return found

    plan = []
    for t, team in enumerate(teams):
        mine = {"j": look_up(pick[t], col)}
        src = source_of(t, col)
        slot = zero
        for c in range(columns):
            slot = slot + jnp.where(c < src, reaches[c], 0)
        mine["slot"] = jnp.minimum(slot, blocks - 1)
        if team[0] == "G":
            f, l = team[1:3]
            mine["I"] = (f, l, place_among(source_of(t, partner(l)), f, 0), place_among(src, f, 4))
            f, l = team[3:5]
        else:
            f, l = team[1:3]
        mine["O"] = (
            f, l, place_among(look_up(dest[t], partner(l)), f, 0), place_among(look_up(dest[t], col), f, 4)
        )
        plan.append(mine)

    pending = []

    def launch(copy):
        copy.start()
        pending.append(copy)

    def to_column(src, dst, key, k, s):
        return pltpu.make_async_remote_copy(
            src_ref=src, dst_ref=dst,
            send_sem=ref[key + ("snd",)].at[k], recv_sem=ref[key + ("rcv",)].at[k],
            device_id={"fsdp": partner(s)}, device_id_type=MESH,
        )

    def to_group(src, dst, key, k, g):
        return pltpu.make_async_remote_copy(
            src_ref=src, dst_ref=dst,
            send_sem=ref[key + ("snd",)].at[k], recv_sem=ref[key + ("rcv",)].at[k],
            device_id={"grp": g}, device_id_type=MESH,
        )

    def route_copy(kind, t, way, k):
        f, l = plan[t][way][:2]
        cand = ref[("cand", t, way, k)]
        if kind == "f":
            return to_column(cand.at[0], cand.at[2], ("f", t, way), k, f)
        if kind == "b":
            return to_column(cand.at[0], cand.at[1], ("b", t, way), k, 1)
        if kind == "bf":
            return to_column(cand.at[2], cand.at[3], ("bf", t, way), k, 1)
        return to_column(ref[("sel", t, way, k)], ref[("last", t, way, k)], ("l", t, way), k, l)

    def enter(t, way, k, piece):
        ref[("cand", t, way, k)][0] = piece
        launch(route_copy("f", t, way, k))
        launch(route_copy("b", t, way, k))

    def relay(t, way, k):
        route_copy("f", t, way, k).wait_recv()
        launch(route_copy("bf", t, way, k))

    def select(t, way, k):
        route_copy("b", t, way, k).wait_recv()
        route_copy("bf", t, way, k).wait_recv()
        ref[("sel", t, way, k)][...] = ref[("cand", t, way, k)][plan[t][way][2]]
        launch(route_copy("l", t, way, k))

    def leave(t, way, k):
        route_copy("l", t, way, k).wait_recv()
        place = plan[t][way][3]
        return jnp.where(
            place == 4, ref[("last", t, way, k)][...], ref[("cand", t, way, k)][jnp.minimum(place, 3)]
        )

    def across_copy(t, way, k, g):
        piece = ref[("all", t, way, k)].at[g]
        return to_group(piece, piece, ("across", t, way), k, across)

    def mate_copy(t, way, k, g, i):
        piece = ref[("all", t, way, k)].at[g]
        return to_group(piece, piece, ("mate%d" % i, t, way), k, mate)

    def share(t, way, k, piece):
        ref[("all", t, way, k)][grp] = piece
        launch(across_copy(t, way, k, grp))
        launch(mate_copy(t, way, k, grp, 0))

    def pass_on(t, way, k):
        across_copy(t, way, k, across).wait_recv()
        launch(mate_copy(t, way, k, across, 1))

    def gathered(t, way, k):
        mate_copy(t, way, k, mate, 0).wait_recv()
        mate_copy(t, way, k, diagonal, 1).wait_recv()

    def whole(t, way, k):
        return ref[("all", t, way, k)][...].reshape(groups * rows, w)

    def dot(a, b):
        return jnp.dot(a, b, preferred_element_type=jnp.float32).astype(out_ref.dtype)

    def home_copy(t, k):
        return to_group(
            ref[("pc", t, "O", k)].at[1 - core], ref[("rcvc", t, "O", k)], ("home", t, "O"), k, mate
        )

    def back_copy(t, k):
        return to_group(
            ref[("sely", t, "O", k)], ref[("rcvy", t, "O", k)], ("back", t, "O"), k, across
        )

    def owner_side(t, k, which):
        return jnp.where(
            owner_core == core, ref[("pc", t, "O", k)][core, which], ref[("rcvc", t, "O", k)][which]
        )

    def offer(t, k, piece_of):
        for g in range(groups):
            ref[("pc", t, "O", k)][g % 2, g // 2] = piece_of(g)
        launch(home_copy(t, k))

    waited = [False, False, False]

    def loaded(n):
        if not waited[n]:
            loads[n].wait()
            waited[n] = True

    def run(name, t, k):
        q = k % chunks
        slot = plan[t]["slot"]
        if name in ("I0", "G0"):
            loaded(0)
            piece = gv[plan[t]["j"], :, cols_of(q)]
            if name == "I0":
                enter(t, "I", k, piece)
            else:
                share(t, "I", k, piece)
        elif name == "I1":
            relay(t, "I", k)
        elif name == "I2":
            select(t, "I", k)
        elif name == "I3":
            share(t, "I", k, leave(t, "I", k))
        elif name in ("I4", "G1"):
            pass_on(t, "I", k)
        elif name == "G2":
            gathered(t, "I", k)
        elif name == "I5":
            loaded(1)
            gathered(t, "I", k)
            ref[("lp", t)][:, cols_of(q)] = dot(lv[slot], whole(t, "I", k))
        elif name == "R":
            loaded(2)
            product = dot(ref[("lp", t)][...], rv[slot, :, cols_of(q)])
            offer(t, k, lambda g: product[g * rows:(g + 1) * rows])
        elif name == "S0":
            n = 1 if k < chunks else 2
            loaded(n)
            table = lv if k < chunks else rv
            offer(t, k, lambda g: table[slot, g * rows:(g + 1) * rows, cols_of(q)])
        elif name == "H":
            home_copy(t, k).wait_recv()
            ref[("sely", t, "O", k)][...] = owner_side(t, k, 1 - half)
            launch(back_copy(t, k))
        elif name == "O0":
            back_copy(t, k).wait_recv()
            mine = owner_side(t, k, half)
            enter(t, "O", k, jnp.where(owner_half == half, mine, ref[("rcvy", t, "O", k)][...]))
        elif name == "O1":
            relay(t, "O", k)
        elif name == "O2":
            select(t, "O", k)
        elif name == "O3":
            piece = leave(t, "O", k)
            if teams[t][0] == "G":
                ref[("fin", t)][:, cols_of(q)] = piece
            elif k < chunks:
                ref[("lrow", t)][:, cols_of(q)] = piece
            else:
                share(t, "O", q, piece)
        elif name == "LG":
            for n in range(chunks):
                ref[("lg", t)][:, cols_of(n)] = dot(ref[("lrow", t)][...], whole(t, "I", n))
        elif name == "O4":
            pass_on(t, "O", q)
        elif name == "O5":
            gathered(t, "O", q)
            ref[("fin", t)][:, cols_of(q)] = dot(ref[("lg", t)][...], whole(t, "O", q))

    pl.semaphore_wait(barrier, 5)
    for step in timetable(teams, chunks):
        run(*step)
    for j in range(blocks):
        value = ref[("fin", 0)][...]
        for t in range(1, blocks):
            value = jnp.where(plan[t]["j"] == j, ref[("fin", t)][...], value)
        out_ref[j] = value
    for n in range(3):
        loaded(n)
    for copy in pending:
        copy.wait_send()


def per_device_fused(gradient, left_factor, right_factor, block_owner):
    blocks, rows, width = gradient.shape
    columns = lax.axis_size("fsdp")
    groups = lax.axis_size("grp")
    far, near = columns // 2, columns // 4
    sides = {"far": (far, near), "near": (near, far)}
    teams = tuple((team[0],) + sum((sides[s] for s in team[1:]), ()) for team in TEAMS)
    held = scratch_of(teams, CHUNKS, blocks, columns, groups, rows, width, gradient.dtype)
    return pl.pallas_call(
        functools.partial(
            preconditioner_kernel, teams, CHUNKS, tuple(held), columns, groups, blocks, rows, width
        ),
        out_shape=jax.ShapeDtypeStruct(gradient.shape, gradient.dtype),
        in_specs=[pl.BlockSpec(memory_space=pltpu.SMEM)] + [pl.BlockSpec(memory_space=pl.ANY)] * 3,
        out_specs=pl.BlockSpec(memory_space=pltpu.VMEM),
        scratch_shapes=list(held.values()),
        compiler_params=pltpu.CompilerParams(
            collective_id=0, has_side_effects=True, vmem_limit_bytes=67043328
        ),
    )(block_owner, gradient, left_factor, right_factor)


def per_device_any(gradient, left_factor, right_factor, block_owner):
    blocks = gradient.shape[0]
    columns = lax.axis_size("fsdp")
    fits = (
        blocks == left_factor.shape[0]
        and blocks == len(TEAMS)
        and lax.axis_size("grp") == 4
        and columns == 8
        and gradient.shape[2] % (CHUNKS * 128) == 0
    )
    body = per_device_fused if fits else per_device
    return body(gradient, left_factor, right_factor, block_owner)


def solution(mesh):
    return jax.shard_map(
        per_device_any,
        mesh=mesh,
        in_specs=(
            P("fsdp", "grp", None),
            P(("fsdp", "grp"), None, None),
            P(("fsdp", "grp"), None, None),
            P(),
        ),
        out_specs=P("fsdp", "grp", None),
        check_vma=False,
    )
```

```python
import functools

import jax
import jax.numpy as jnp
from jax import lax
from jax.experimental import pallas as pl
from jax.experimental.pallas import tpu as pltpu
from jax.sharding import PartitionSpec as P

MESH = pl.DeviceIdType.MESH
CHUNKS = 4
SENT = 5
TEAMS = (('G', 'far', 'near'), ('F', 'far'), ('F', 'near'))
GRADIENT_STEPS = ("I0", "I1", "I2", "I3", "I4", "I5", "R", "H", "O0", "O1", "O2", "O3")
WHEN = {
    ('I0', 0): (0, 1, 2, 3),
    ('S0', 1): (4, 5, 6, 7, 8, 9, 13, 18),
    ('S0', 2): (10, 25, 28, 38, 44, 51, 59, 72),
    ('H', 1): (11, 12, 14, 15, 16, 17, 22, 27),
    ('H', 2): (19, 30, 33, 41, 49, 57, 69, 77),
    ('G0', 1): (20, 21, 23, 24),
    ('I1', 0): (26, 32, 34, 39),
    ('O0', 1): (29, 31, 35, 37, 40, 42, 53, 67),
    ('I2', 0): (36, 43, 47, 61),
    ('I3', 0): (45, 52, 65, 75),
    ('O0', 2): (46, 64, 74, 81, 89, 94, 100, 106),
    ('O1', 1): (48, 56, 62, 70, 76, 78, 86, 95),
    ('G1', 1): (50, 54, 60, 63),
    ('G2', 1): (55, 58, 68, 73),
    ('O1', 2): (66, 93, 97, 102, 109, 116, 123, 130),
    ('O2', 1): (71, 80, 85, 96, 103, 108, 120, 128),
    ('I4', 0): (79, 87, 99, 105),
    ('G0', 2): (82, 83, 84, 91),
    ('O3', 1): (88, 101, 107, 118, 125, 135, 137, 144),
    ('O2', 2): (90, 119, 131, 138, 143, 147, 152, 154),
    ('I5', 0): (92, 98, 104, 111),
    ('G1', 2): (110, 112, 115, 117),
    ('O3', 2): (113, 141, 151, 156, 163, 167, 170, 172),
    ('R', 0): (114, 121, 126, 132),
    ('LG', 1): (122,),
    ('H', 0): (124, 129, 134, 139),
    ('G2', 2): (127, 133, 136, 146),
    ('O0', 0): (140, 145, 150, 159),
    ('O4', 1): (142, 148, 157, 161),
    ('O5', 1): (149, 155, 162, 165),
    ('O1', 0): (153, 160, 164, 168),
    ('LG', 2): (158,),
    ('O2', 0): (166, 169, 173, 174),
    ('O4', 2): (171, 176, 179, 180),
    ('O5', 2): (175, 178, 182, 183),
    ('O3', 0): (177, 181, 184, 185),
}


def per_device(gradient, left_factor, right_factor, block_owner):
    local_blocks = gradient.shape[0]
    piece_rows = gradient.shape[1]
    block_width = gradient.shape[2]
    slot_count = left_factor.shape[0]
    columns = lax.axis_size("fsdp")
    groups = lax.axis_size("grp")
    column = lax.axis_index("fsdp")
    owners_all = block_owner.reshape(columns, local_blocks)
    dest_column = owners_all // groups
    dest_group = owners_all % groups
    mine_column = lax.dynamic_index_in_dim(dest_column, column, 0, keepdims=False)
    column_ids = jnp.arange(columns, dtype=jnp.int32)
    matching = mine_column[None, :] == column_ids[:, None]
    pick_send = matching.astype(jnp.bfloat16)
    outgoing = jnp.einsum(
        "cj,jrd->crd", pick_send, gradient, preferred_element_type=jnp.float32
    ).astype(jnp.bfloat16)
    arrived = lax.all_to_all(
        outgoing.reshape(columns * piece_rows, block_width),
        "fsdp",
        split_axis=0,
        concat_axis=0,
        tiled=True,
    )
    arrived = arrived.reshape(columns, piece_rows, block_width)
    toward = dest_column == column
    live_source = jnp.sum(toward.astype(jnp.int32), axis=1) > 0
    target = jnp.sum(jnp.where(toward, dest_group, 0), axis=1)
    same_owner = (target[None, :] == target[:, None]) & live_source[None, :] & live_source[:, None]
    before = column_ids[None, :] < column_ids[:, None]
    rank_slot = jnp.sum((same_owner & before).astype(jnp.int32), axis=1)
    group_ids = jnp.arange(groups, dtype=jnp.int32)
    slot_ids = jnp.arange(slot_count, dtype=jnp.int32)
    routing = (
        live_source[None, None, :]
        & (target[None, None, :] == group_ids[:, None, None])
        & (rank_slot[None, None, :] == slot_ids[None, :, None])
    )
    routing = routing.astype(jnp.bfloat16)
    packed = jnp.einsum(
        "oks,srd->kord", routing, arrived, preferred_element_type=jnp.float32
    ).astype(jnp.bfloat16)
    packed = packed.reshape(slot_count, groups * piece_rows, block_width)
    blocks = lax.all_to_all(packed, "grp", split_axis=1, concat_axis=1, tiled=True)
    left_product = jnp.einsum(
        "kab,kbc->kac", left_factor, blocks, preferred_element_type=jnp.float32
    ).astype(jnp.bfloat16)
    result = jnp.einsum(
        "kab,kbc->kac", left_product, right_factor, preferred_element_type=jnp.float32
    ).astype(jnp.bfloat16)
    returned = lax.all_to_all(result, "grp", split_axis=1, concat_axis=1, tiled=True)
    returned = returned.reshape(slot_count, groups, piece_rows, block_width)
    unpacked = jnp.einsum(
        "oks,kord->srd", routing, returned, preferred_element_type=jnp.float32
    ).astype(jnp.bfloat16)
    homeward = lax.all_to_all(
        unpacked.reshape(columns * piece_rows, block_width),
        "fsdp",
        split_axis=0,
        concat_axis=0,
        tiled=True,
    )
    homeward = homeward.reshape(columns, piece_rows, block_width)
    return jnp.einsum(
        "cj,crd->jrd", pick_send, homeward, preferred_element_type=jnp.float32
    ).astype(jnp.bfloat16)


def stages_of(team, chunks):
    if team[0] == "G":
        return [(name, chunks) for name in GRADIENT_STEPS]
    found = [(name, chunks) for name in ("G0", "G1", "G2")]
    found += [(name, 2 * chunks) for name in ("S0", "H", "O0", "O1", "O2", "O3")]
    return found + [("LG", 1), ("O4", chunks), ("O5", chunks)]


def timetable(teams, chunks):
    steps = []
    for t, team in enumerate(teams):
        for name, count in stages_of(team, chunks):
            first = chunks if name in ("O4", "O5") else 0
            for i in range(count):
                steps.append((WHEN[(name, t)][i], len(steps), name, t, first + i))
    return [step[2:] for step in sorted(steps)]


def scratch_of(teams, chunks, blocks, columns, groups, rows, width, dtype):
    w = width // chunks
    vmem = lambda *shape: pltpu.VMEM(shape, dtype)
    dma = pltpu.SemaphoreType.DMA
    held = {
        "gv": vmem(blocks, rows, width),
        "lv": vmem(blocks, width, width),
        "rv": vmem(blocks, width, width),
        "load": dma((3,)),
        "sent": dma((SENT,)),
        "power": pltpu.SMEM((columns,), jnp.int32),
    }

    def copies(key, count):
        held[key + ("rcv",)] = dma((count,))

    def route(key, count):
        for k in range(count):
            held[("cand",) + key + (k,)] = vmem(4, rows, w)
            held[("last",) + key + (k,)] = vmem(rows, w)
            held[("sel",) + key + (k,)] = vmem(rows, w)
        for name in ("f", "b", "l"):
            copies((name,) + key, count)

    def gather(key, count):
        for k in range(count):
            held[("all",) + key + (k,)] = vmem(groups, rows, w)
        for name in ("across", "mate"):
            copies((name,) + key, count)

    def scatter(key, count):
        for k in range(count):
            held[("pc",) + key + (k,)] = vmem(2, 2, rows, w)
            held[("rcvc",) + key + (k,)] = vmem(2, rows, w)
            held[("sely",) + key + (k,)] = vmem(rows, w)
            held[("rcvy",) + key + (k,)] = vmem(rows, w)
        for name in ("home", "back"):
            copies((name,) + key, count)

    for t, team in enumerate(teams):
        held[("fin", t)] = vmem(rows, width)
        if team[0] == "G":
            route((t, "I"), chunks)
            gather((t, "I"), chunks)
            held[("lp", t)] = vmem(width, width)
            scatter((t, "O"), chunks)
            route((t, "O"), chunks)
        else:
            gather((t, "I"), chunks)
            scatter((t, "O"), 2 * chunks)
            route((t, "O"), 2 * chunks)
            gather((t, "O"), chunks)
            held[("lrow", t)] = vmem(rows, width)
            held[("lg", t)] = vmem(rows, width)
    return held


def preconditioner_kernel(
    teams, chunks, names, columns, groups, blocks, rows, width,
    owner_ref, g_hbm, l_hbm, r_hbm, out_ref, *rest,
):
    ref = dict(zip(names, rest))
    col = lax.axis_index("fsdp")
    grp = lax.axis_index("grp")
    core = grp % 2
    half = grp // 2
    mate = half * 2 + (1 - core)
    across = (1 - half) * 2 + core
    w = width // chunks
    zero = jnp.int32(0)

    def cols_of(q):
        return slice(q * w, (q + 1) * w)

    def partner(s):
        d, b = 0, 1
        while b < columns:
            v = (col // b) % 2
            d, b = d + b * ((1 - v) if s & b else v), 2 * b
        return d

    gv, lv, rv = ref["gv"], ref["lv"], ref["rv"]
    loads = [
        pltpu.make_async_copy(g_hbm, gv, ref["load"].at[0]),
        pltpu.make_async_copy(l_hbm, lv, ref["load"].at[1]),
        pltpu.make_async_copy(r_hbm, rv, ref["load"].at[2]),
    ]
    for load in loads:
        load.start()

    far, near = columns // 2, columns // 4
    barrier = pltpu.get_barrier_semaphore()
    for s in (1, near, far):
        pl.semaphore_signal(barrier, inc=1, device_id={"fsdp": partner(s)}, device_id_type=MESH)
    for g in (mate, across):
        pl.semaphore_signal(barrier, inc=1, device_id={"grp": g}, device_id_type=MESH)

    def look_up(table, index):
        found = zero
        for n, value in enumerate(table):
            found = jnp.where(index == n, value, found)
        return found

    power = ref["power"]
    for d in range(columns):
        power[d] = jnp.int32(2 ** d)
    to = [[owner_ref[c * blocks + j] // groups for j in range(blocks)] for c in range(columns)]
    left_over = [[(jnp.int32(j), to[c][j], power[to[c][j]]) for j in range(blocks)] for c in range(columns)]
    pick, dest = [], []
    full = 2 ** columns - 1
    while len(left_over[0]) > 1:
        m = len(left_over[0])
        count = m ** columns
        tall = -(-count // 1024) * 8
        inverse = -(-(2 ** 17) // m)
        index = (
            lax.broadcasted_iota(jnp.int32, (tall, 128), 0) * 128
            + lax.broadcasted_iota(jnp.int32, (tall, 128), 1)
        )
        rest_of, reach = index, jnp.zeros((tall, 128), jnp.int32)
        for c in range(columns):
            upper = (rest_of * inverse) >> 17
            digit = rest_of - upper * m
            bit = jnp.full((tall, 128), left_over[c][m - 1][2], jnp.int32)
            for i in range(m - 1):
                bit = jnp.where(digit == i, left_over[c][i][2], bit)
            reach, rest_of = reach | bit, upper
        chosen = jnp.min(jnp.where((reach == full) & (index < count), index, count - 1))
        pick_t, dest_t = [], []
        for c in range(columns):
            upper = (chosen * inverse) >> 17
            digit, chosen = chosen - upper * m, upper
            pick_t.append(look_up([e[0] for e in left_over[c]], digit))
            dest_t.append(look_up([e[1] for e in left_over[c]], digit))
            left_over[c] = [
                tuple(jnp.where(digit <= i, b, a) for a, b in zip(left_over[c][i], left_over[c][i + 1]))
                for i in range(m - 1)
            ]
        pick.append(pick_t)
        dest.append(dest_t)
    pick.append([left_over[c][0][0] for c in range(columns)])
    dest.append([left_over[c][0][1] for c in range(columns)])

    owner_group = zero
    for c in range(columns):
        for j in range(blocks):
            owner_group = jnp.where(to[c][j] == col, owner_ref[c * blocks + j] % groups, owner_group)
    owner_core = owner_group % 2
    owner_half = owner_group // 2
    reaches = []
    for c in range(columns):
        hit = zero
        for j in range(blocks):
            hit = jnp.where(to[c][j] == col, 1, hit)
        reaches.append(hit)

    def source_of(t, d):
        found = zero
        for c in range(columns):
            found = jnp.where(dest[t][c] == d, c, found)
        return found

    def place_among(wanted, f, other):
        found = jnp.int32(other)
        for n, s in enumerate((0, 1, f, f + 1)):
            found = jnp.where(wanted == partner(s), n, found)
        return found

    plan = []
    for t, team in enumerate(teams):
        mine = {"j": look_up(pick[t], col)}
        src = source_of(t, col)
        slot = zero
        for c in range(columns):
            slot = slot + jnp.where(c < src, reaches[c], 0)
        mine["slot"] = jnp.minimum(slot, blocks - 1)
        if team[0] == "G":
            f, l = team[1:3]
            mine["I"] = (f, l, place_among(source_of(t, partner(l)), f, 0), place_among(src, f, 4))
            f, l = team[3:5]
        else:
            f, l = team[1:3]
        mine["O"] = (
            f, l, place_among(look_up(dest[t], partner(l)), f, 0), place_among(look_up(dest[t], col), f, 4)
        )
        plan.append(mine)

    most = blocks * width // (rows // chunks)
    sent, now = [0], [0]

    def launch(copy, pieces=1):
        if max(most - n for n in sent) < pieces:
            sent.append(0)
        now[0] = next(n for n, held in enumerate(sent) if held + pieces <= most)
        copy().start()
        sent[now[0]] += pieces

    def all_sent():
        step = rows // chunks
        for n, pieces in enumerate(sent):
            over = next(b for b in range(1, blocks + 1) if pieces % b == 0 and pieces // b * step <= width)
            view = lv.at[0:over, 0:pieces // over * step]
            pltpu.make_async_copy(view, view, ref["sent"].at[n]).wait()

    def remote(src, dst, key, k, device):
        return pltpu.make_async_remote_copy(
            src_ref=src, dst_ref=dst,
            send_sem=ref["sent"].at[now[0]], recv_sem=ref[key + ("rcv",)].at[k],
            device_id=device, device_id_type=MESH,
        )

    def to_column(src, dst, key, k, s):
        return remote(src, dst, key, k, {"fsdp": partner(s)})

    def to_group(src, dst, key, k, g):
        return remote(src, dst, key, k, {"grp": g})

    def both_arrived(pair, key, k):
        pltpu.make_async_copy(pair, pair, ref[key + ("rcv",)].at[k]).wait()

    def route_copy(kind, t, way, k):
        f, l = plan[t][way][:2]
        cand = ref[("cand", t, way, k)]
        if kind == "f":
            return to_column(cand.at[0], cand.at[2], ("f", t, way), k, f)
        if kind == "b":
            return to_column(cand.at[0], cand.at[1], ("b", t, way), k, 1)
        if kind == "bf":
            return to_column(cand.at[2], cand.at[3], ("b", t, way), k, 1)
        return to_column(ref[("sel", t, way, k)], ref[("last", t, way, k)], ("l", t, way), k, l)

    def enter(t, way, k, piece):
        ref[("cand", t, way, k)][0] = piece
        launch(lambda: route_copy("f", t, way, k))
        launch(lambda: route_copy("b", t, way, k))

    def relay(t, way, k):
        route_copy("f", t, way, k).wait_recv()
        launch(lambda: route_copy("bf", t, way, k))

    def select(t, way, k):
        both_arrived(ref[("cand", t, way, k)].at[0:2], ("b", t, way), k)
        ref[("sel", t, way, k)][...] = ref[("cand", t, way, k)][plan[t][way][2]]
        launch(lambda: route_copy("l", t, way, k))

    def leave(t, way, k):
        route_copy("l", t, way, k).wait_recv()
        place = plan[t][way][3]
        return jnp.where(
            place == 4, ref[("last", t, way, k)][...], ref[("cand", t, way, k)][jnp.minimum(place, 3)]
        )

    def across_copy(t, way, k, g):
        piece = ref[("all", t, way, k)].at[g]
        return to_group(piece, piece, ("across", t, way), k, across)

    def mate_copy(t, way, k, g):
        piece = ref[("all", t, way, k)].at[g]
        return to_group(piece, piece, ("mate", t, way), k, mate)

    def share(t, way, k, piece):
        ref[("all", t, way, k)][grp] = piece
        launch(lambda: across_copy(t, way, k, grp))
        launch(lambda: mate_copy(t, way, k, grp))

    def pass_on(t, way, k):
        across_copy(t, way, k, across).wait_recv()
        launch(lambda: mate_copy(t, way, k, across))

    def gathered(t, way, k):
        both_arrived(ref[("all", t, way, k)].at[0:2], ("mate", t, way), k)

    def whole(t, way, k):
        return ref[("all", t, way, k)][...].reshape(groups * rows, w)

    def dot(a, b):
        return jnp.dot(a, b, preferred_element_type=jnp.float32).astype(out_ref.dtype)

    def home_copy(t, k):
        return to_group(
            ref[("pc", t, "O", k)].at[1 - core], ref[("rcvc", t, "O", k)], ("home", t, "O"), k, mate
        )

    def back_copy(t, k):
        return to_group(
            ref[("sely", t, "O", k)], ref[("rcvy", t, "O", k)], ("back", t, "O"), k, across
        )

    def owner_side(t, k, which):
        return jnp.where(
            owner_core == core, ref[("pc", t, "O", k)][core, which], ref[("rcvc", t, "O", k)][which]
        )

    def offer(t, k, piece_of):
        for g in range(groups):
            ref[("pc", t, "O", k)][g % 2, g // 2] = piece_of(g)
        launch(lambda: home_copy(t, k), 2)

    waited = [False, False, False]

    def loaded(n):
        if not waited[n]:
            loads[n].wait()
            waited[n] = True

    def run(name, t, k):
        q = k % chunks
        slot = plan[t]["slot"]
        if name in ("I0", "G0"):
            loaded(0)
            piece = gv[plan[t]["j"], :, cols_of(q)]
            if name == "I0":
                enter(t, "I", k, piece)
            else:
                share(t, "I", k, piece)
        elif name == "I1":
            relay(t, "I", k)
        elif name == "I2":
            select(t, "I", k)
        elif name == "I3":
            share(t, "I", k, leave(t, "I", k))
        elif name in ("I4", "G1"):
            pass_on(t, "I", k)
        elif name == "G2":
            gathered(t, "I", k)
        elif name == "I5":
            loaded(1)
            gathered(t, "I", k)
            ref[("lp", t)][:, cols_of(q)] = dot(lv[slot], whole(t, "I", k))
        elif name == "R":
            loaded(2)
            product = dot(ref[("lp", t)][...], rv[slot, :, cols_of(q)])
            offer(t, k, lambda g: product[g * rows:(g + 1) * rows])
        elif name == "S0":
            n = 1 if k < chunks else 2
            loaded(n)
            table = lv if k < chunks else rv
            offer(t, k, lambda g: table[slot, g * rows:(g + 1) * rows, cols_of(q)])
        elif name == "H":
            home_copy(t, k).wait_recv()
            ref[("sely", t, "O", k)][...] = owner_side(t, k, 1 - half)
            launch(lambda: back_copy(t, k))
        elif name == "O0":
            back_copy(t, k).wait_recv()
            mine = owner_side(t, k, half)
            enter(t, "O", k, jnp.where(owner_half == half, mine, ref[("rcvy", t, "O", k)][...]))
        elif name == "O1":
            relay(t, "O", k)
        elif name == "O2":
            select(t, "O", k)
        elif name == "O3":
            piece = leave(t, "O", k)
            if teams[t][0] == "G":
                ref[("fin", t)][:, cols_of(q)] = piece
            elif k < chunks:
                ref[("lrow", t)][:, cols_of(q)] = piece
            else:
                share(t, "O", q, piece)
        elif name == "LG":
            for n in range(chunks):
                ref[("lg", t)][:, cols_of(n)] = dot(ref[("lrow", t)][...], whole(t, "I", n))
        elif name == "O4":
            pass_on(t, "O", q)
        elif name == "O5":
            gathered(t, "O", q)
            ref[("fin", t)][:, cols_of(q)] = dot(ref[("lg", t)][...], whole(t, "O", q))

    pl.semaphore_wait(barrier, 5)
    for step in timetable(teams, chunks):
        run(*step)
    for j in range(blocks):
        value = ref[("fin", 0)][...]
        for t in range(1, blocks):
            value = jnp.where(plan[t]["j"] == j, ref[("fin", t)][...], value)
        out_ref[j] = value
    for n in range(3):
        loaded(n)
    all_sent()


def per_device_fused(gradient, left_factor, right_factor, block_owner):
    blocks, rows, width = gradient.shape
    columns = lax.axis_size("fsdp")
    groups = lax.axis_size("grp")
    far, near = columns // 2, columns // 4
    sides = {"far": (far, near), "near": (near, far)}
    teams = tuple((team[0],) + sum((sides[s] for s in team[1:]), ()) for team in TEAMS)
    held = scratch_of(teams, CHUNKS, blocks, columns, groups, rows, width, gradient.dtype)
    return pl.pallas_call(
        functools.partial(
            preconditioner_kernel, teams, CHUNKS, tuple(held), columns, groups, blocks, rows, width
        ),
        out_shape=jax.ShapeDtypeStruct(gradient.shape, gradient.dtype),
        in_specs=[pl.BlockSpec(memory_space=pltpu.SMEM)] + [pl.BlockSpec(memory_space=pl.ANY)] * 3,
        out_specs=pl.BlockSpec(memory_space=pltpu.VMEM),
        scratch_shapes=list(held.values()),
        compiler_params=pltpu.CompilerParams(
            collective_id=0, has_side_effects=True, vmem_limit_bytes=67043328
        ),
    )(block_owner, gradient, left_factor, right_factor)


def per_device_any(gradient, left_factor, right_factor, block_owner):
    blocks = gradient.shape[0]
    columns = lax.axis_size("fsdp")
    fits = (
        blocks == left_factor.shape[0]
        and blocks == len(TEAMS)
        and lax.axis_size("grp") == 4
        and columns == 8
        and gradient.shape[2] % (CHUNKS * 128) == 0
    )
    body = per_device_fused if fits else per_device
    return body(gradient, left_factor, right_factor, block_owner)


def solution(mesh):
    return jax.shard_map(
        per_device_any,
        mesh=mesh,
        in_specs=(
            P("fsdp", "grp", None),
            P(("fsdp", "grp"), None, None),
            P(("fsdp", "grp"), None, None),
            P(),
        ),
        out_specs=P("fsdp", "grp", None),
        check_vma=False,
    )
```

```python
import functools
import math

import jax
import jax.numpy as jnp
from jax import lax
from jax.experimental import pallas as pl
from jax.experimental.pallas import tpu as pltpu
from jax.sharding import PartitionSpec as P

MESH = pl.DeviceIdType.MESH
CHUNKS = 4
COARSE = 2
SENT = 5
TEAMS = (('G', ('H', 'far'), ('H', 'near')), ('F', ('H', 'far')), ('F', ('H', 'near')))
ROUTE_STEPS = {"H": "0123", "X": "012X3"}
WHEN = {
    ('I0', 0): (0, 1, 2, 3),
    ('S0', 1): (4, 5, 6, 7, 8, 9, 13, 18),
    ('S0', 2): (10, 25, 28, 38, 44, 51, 59, 72),
    ('H', 1): (11, 12, 14, 15, 16, 17, 22, 27),
    ('H', 2): (19, 30, 33, 41, 49, 57, 69, 77),
    ('G0', 1): (20, 21, 23, 24),
    ('I1', 0): (26, 32, 34, 39),
    ('O0', 1): (29, 31, 35, 37, 40, 42, 53, 67),
    ('I2', 0): (36, 43, 47, 61),
    ('I3', 0): (45, 52, 65, 75),
    ('O0', 2): (46, 64, 74, 81, 89, 94, 100, 106),
    ('O1', 1): (48, 56, 62, 70, 76, 78, 86, 95),
    ('G1', 1): (50, 54, 60, 63),
    ('G2', 1): (55, 58, 68, 73),
    ('O1', 2): (66, 93, 97, 102, 109, 116, 123, 130),
    ('O2', 1): (71, 80, 85, 96, 103, 108, 120, 128),
    ('I4', 0): (79, 87, 99, 105),
    ('G0', 2): (82, 83, 84, 91),
    ('O3', 1): (88, 101, 107, 118, 125, 135, 137, 144),
    ('O2', 2): (90, 119, 131, 138, 143, 147, 152, 154),
    ('I5', 0): (92, 98, 104, 111),
    ('G1', 2): (110, 112, 115, 117),
    ('O3', 2): (113, 141, 151, 156, 163, 167, 170, 172),
    ('R', 0): (114, 121, 126, 132),
    ('LG', 1): (122,),
    ('H', 0): (124, 129, 134, 139),
    ('G2', 2): (127, 133, 136, 146),
    ('O0', 0): (140, 145, 150, 159),
    ('O4', 1): (142, 148, 157, 161),
    ('O5', 1): (149, 155, 162, 165),
    ('O1', 0): (153, 160, 164, 168),
    ('LG', 2): (158,),
    ('O2', 0): (166, 169, 173, 174),
    ('O4', 2): (171, 176, 179, 180),
    ('O5', 2): (175, 178, 182, 183),
    ('O3', 0): (177, 181, 184, 185),
}


def per_device(gradient, left_factor, right_factor, block_owner):
    local_blocks = gradient.shape[0]
    piece_rows = gradient.shape[1]
    block_width = gradient.shape[2]
    slot_count = left_factor.shape[0]
    columns = lax.axis_size("fsdp")
    groups = lax.axis_size("grp")
    column = lax.axis_index("fsdp")
    owners_all = block_owner.reshape(columns, local_blocks)
    dest_column = owners_all // groups
    dest_group = owners_all % groups
    mine_column = lax.dynamic_index_in_dim(dest_column, column, 0, keepdims=False)
    column_ids = jnp.arange(columns, dtype=jnp.int32)
    matching = mine_column[None, :] == column_ids[:, None]
    pick_send = matching.astype(jnp.bfloat16)
    outgoing = jnp.einsum(
        "cj,jrd->crd", pick_send, gradient, preferred_element_type=jnp.float32
    ).astype(jnp.bfloat16)
    arrived = lax.all_to_all(
        outgoing.reshape(columns * piece_rows, block_width),
        "fsdp",
        split_axis=0,
        concat_axis=0,
        tiled=True,
    )
    arrived = arrived.reshape(columns, piece_rows, block_width)
    toward = dest_column == column
    live_source = jnp.sum(toward.astype(jnp.int32), axis=1) > 0
    target = jnp.sum(jnp.where(toward, dest_group, 0), axis=1)
    same_owner = (target[None, :] == target[:, None]) & live_source[None, :] & live_source[:, None]
    before = column_ids[None, :] < column_ids[:, None]
    rank_slot = jnp.sum((same_owner & before).astype(jnp.int32), axis=1)
    group_ids = jnp.arange(groups, dtype=jnp.int32)
    slot_ids = jnp.arange(slot_count, dtype=jnp.int32)
    routing = (
        live_source[None, None, :]
        & (target[None, None, :] == group_ids[:, None, None])
        & (rank_slot[None, None, :] == slot_ids[None, :, None])
    )
    routing = routing.astype(jnp.bfloat16)
    packed = jnp.einsum(
        "oks,srd->kord", routing, arrived, preferred_element_type=jnp.float32
    ).astype(jnp.bfloat16)
    packed = packed.reshape(slot_count, groups * piece_rows, block_width)
    blocks = lax.all_to_all(packed, "grp", split_axis=1, concat_axis=1, tiled=True)
    left_product = jnp.einsum(
        "kab,kbc->kac", left_factor, blocks, preferred_element_type=jnp.float32
    ).astype(jnp.bfloat16)
    result = jnp.einsum(
        "kab,kbc->kac", left_product, right_factor, preferred_element_type=jnp.float32
    ).astype(jnp.bfloat16)
    returned = lax.all_to_all(result, "grp", split_axis=1, concat_axis=1, tiled=True)
    returned = returned.reshape(slot_count, groups, piece_rows, block_width)
    unpacked = jnp.einsum(
        "oks,kord->srd", routing, returned, preferred_element_type=jnp.float32
    ).astype(jnp.bfloat16)
    homeward = lax.all_to_all(
        unpacked.reshape(columns * piece_rows, block_width),
        "fsdp",
        split_axis=0,
        concat_axis=0,
        tiled=True,
    )
    homeward = homeward.reshape(columns, piece_rows, block_width)
    return jnp.einsum(
        "cj,crd->jrd", pick_send, homeward, preferred_element_type=jnp.float32
    ).astype(jnp.bfloat16)


def stages_of(team, chunks):
    if team[0] == "G":
        steps = [w + n for w, way in zip("IO", team[1:]) for n in ROUTE_STEPS[way[0]]]
        return [(name, chunks) for name in steps + ["I4", "I5", "R", "H"]]
    steps = ["S0", "H"] + ["O" + n for n in ROUTE_STEPS[team[1][0]]]
    found = [(name, chunks) for name in ("G0", "G1", "G2", "O4", "O5")]
    return found + [(name, 2 * chunks) for name in steps] + [("LG", 1)]


def timetable(teams, chunks):
    steps = []
    for t, team in enumerate(teams):
        for name, count in stages_of(team, chunks):
            first = chunks if name in ("O4", "O5") else 0
            for i in range(count):
                steps.append((WHEN[(name, t)][i], len(steps), name, t, first + i))
    return [step[2:] for step in sorted(steps)]


def scratch_of(teams, chunks, blocks, columns, groups, rows, width, dtype):
    w = width // chunks
    vmem = lambda *shape: pltpu.VMEM(shape, dtype)
    dma = pltpu.SemaphoreType.DMA
    held = {
        "gv": vmem(blocks, rows, width),
        "lv": vmem(blocks, width, width),
        "rv": vmem(blocks, width, width),
        "load": dma((3,)),
        "sent": dma((SENT,)),
        "power": pltpu.SMEM((columns,), jnp.int32),
    }

    def copies(key, count):
        held[key + ("rcv",)] = dma((count,))

    def route(key, count, kind):
        for k in range(count):
            if kind == "H":
                held[("cand",) + key + (k,)] = vmem(4, rows, w)
                held[("last",) + key + (k,)] = vmem(rows, w)
                held[("sel",) + key + (k,)] = vmem(rows, w)
            else:
                held[("cand",) + key + (k,)] = vmem(4, rows // 2, w)
                held[("last",) + key + (k,)] = vmem(2, rows // 2, w)
                held[("sel",) + key + (k,)] = vmem(2, rows // 2, w)
                for name in ("give", "keep", "hand", "take"):
                    held[(name,) + key + (k,)] = vmem(rows // 2, w)
        for name in ("f", "b", "l") if kind == "H" else ("p", "f", "l", "e"):
            copies((name,) + key, count)

    def gather(key, count):
        for k in range(count):
            held[("all",) + key + (k,)] = vmem(groups, rows, w)
        for name in ("across", "mate"):
            copies((name,) + key, count)

    def scatter(key, count):
        for k in range(count):
            held[("pc",) + key + (k,)] = vmem(2, 2, rows, w)
            held[("rcvc",) + key + (k,)] = vmem(2, rows, w)
            held[("sely",) + key + (k,)] = vmem(rows, w)
            held[("rcvy",) + key + (k,)] = vmem(rows, w)
        for name in ("home", "back"):
            copies((name,) + key, count)

    for t, team in enumerate(teams):
        held[("fin", t)] = vmem(rows, width)
        if team[0] == "G":
            route((t, "I"), chunks, team[1][0])
            gather((t, "I"), chunks)
            held[("lp", t)] = vmem(width, width)
            scatter((t, "O"), chunks)
            route((t, "O"), chunks, team[2][0])
        else:
            gather((t, "I"), chunks)
            scatter((t, "O"), 2 * chunks)
            route((t, "O"), 2 * chunks, team[1][0])
            gather((t, "O"), chunks)
            held[("lrow", t)] = vmem(rows, width)
            held[("lg", t)] = vmem(rows, width)
    return held


def preconditioner_kernel(
    teams, chunks, names, columns, groups, blocks, rows, width,
    owner_ref, g_hbm, l_hbm, r_hbm, out_ref, *rest,
):
    ref = dict(zip(names, rest))
    col = lax.axis_index("fsdp")
    grp = lax.axis_index("grp")
    core = grp % 2
    half = grp // 2
    mate = half * 2 + (1 - core)
    across = (1 - half) * 2 + core
    w = width // chunks
    zero = jnp.int32(0)

    def cols_of(q):
        return slice(q * w, (q + 1) * w)

    def partner(s):
        d, b = 0, 1
        while b < columns:
            v = (col // b) % 2
            d, b = d + b * ((1 - v) if s & b else v), 2 * b
        return d

    gv, lv, rv = ref["gv"], ref["lv"], ref["rv"]
    loads = [
        pltpu.make_async_copy(g_hbm, gv, ref["load"].at[0]),
        pltpu.make_async_copy(l_hbm, lv, ref["load"].at[1]),
        pltpu.make_async_copy(r_hbm, rv, ref["load"].at[2]),
    ]
    for load in loads:
        load.start()

    far, near = columns // 2, columns // 4
    barrier = pltpu.get_barrier_semaphore()
    for s in (1, near, far):
        pl.semaphore_signal(barrier, inc=1, device_id={"fsdp": partner(s)}, device_id_type=MESH)
    for g in (mate, across):
        pl.semaphore_signal(barrier, inc=1, device_id={"grp": g}, device_id_type=MESH)

    def look_up(table, index):
        found = zero
        for n, value in enumerate(table):
            found = jnp.where(index == n, value, found)
        return found

    power = ref["power"]
    for d in range(columns):
        power[d] = jnp.int32(2 ** d)
    to = [[owner_ref[c * blocks + j] // groups for j in range(blocks)] for c in range(columns)]
    left_over = [[(jnp.int32(j), to[c][j], power[to[c][j]]) for j in range(blocks)] for c in range(columns)]
    pick, dest = [], []
    full = 2 ** columns - 1
    while len(left_over[0]) > 1:
        m = len(left_over[0])
        count = m ** columns
        tall = -(-count // 1024) * 8
        inverse = -(-(2 ** 17) // m)
        index = (
            lax.broadcasted_iota(jnp.int32, (tall, 128), 0) * 128
            + lax.broadcasted_iota(jnp.int32, (tall, 128), 1)
        )
        rest_of, reach = index, jnp.zeros((tall, 128), jnp.int32)
        for c in range(columns):
            upper = (rest_of * inverse) >> 17
            digit = rest_of - upper * m
            bit = jnp.full((tall, 128), left_over[c][m - 1][2], jnp.int32)
            for i in range(m - 1):
                bit = jnp.where(digit == i, left_over[c][i][2], bit)
            reach, rest_of = reach | bit, upper
        chosen = jnp.min(jnp.where((reach == full) & (index < count), index, count - 1))
        pick_t, dest_t = [], []
        for c in range(columns):
            upper = (chosen * inverse) >> 17
            digit, chosen = chosen - upper * m, upper
            pick_t.append(look_up([e[0] for e in left_over[c]], digit))
            dest_t.append(look_up([e[1] for e in left_over[c]], digit))
            left_over[c] = [
                tuple(jnp.where(digit <= i, b, a) for a, b in zip(left_over[c][i], left_over[c][i + 1]))
                for i in range(m - 1)
            ]
        pick.append(pick_t)
        dest.append(dest_t)
    pick.append([left_over[c][0][0] for c in range(columns)])
    dest.append([left_over[c][0][1] for c in range(columns)])

    owner_group = zero
    for c in range(columns):
        for j in range(blocks):
            owner_group = jnp.where(to[c][j] == col, owner_ref[c * blocks + j] % groups, owner_group)
    owner_core = owner_group % 2
    owner_half = owner_group // 2
    reaches = []
    for c in range(columns):
        hit = zero
        for j in range(blocks):
            hit = jnp.where(to[c][j] == col, 1, hit)
        reaches.append(hit)

    def source_of(t, d):
        found = zero
        for c in range(columns):
            found = jnp.where(dest[t][c] == d, c, found)
        return found

    def place_among(wanted, f, other):
        found = jnp.int32(other)
        for n, s in enumerate((0, 1, f, f + 1)):
            found = jnp.where(wanted == partner(s), n, found)
        return found

    side = col % 2

    def route_plan(way, origin):
        kind, f, l = way
        if kind == "H":
            return kind, f, l, place_among(origin(partner(l)), f, 0), place_among(origin(col), f, 4)
        there = partner(l) - side
        held_by = (col - side, col - side + 1, partner(f) - side, partner(f) - side + 1)

        def place(d, other):
            found, wanted = jnp.int32(other), origin(d)
            for n, c in enumerate(held_by):
                found = jnp.where(wanted == c, n, found)
            return found

        return kind, f, l, place(there, 0), place(there + 1, 0), place(col, 4), place(partner(1), 4)

    plan = []
    for t, team in enumerate(teams):
        mine = {"j": look_up(pick[t], col)}
        src = source_of(t, col)
        slot = zero
        for c in range(columns):
            slot = slot + jnp.where(c < src, reaches[c], 0)
        mine["slot"] = jnp.minimum(slot, blocks - 1)
        if team[0] == "G":
            mine["I"] = route_plan(team[1], functools.partial(source_of, t))
        mine["O"] = route_plan(team[-1], functools.partial(look_up, dest[t]))
        plan.append(mine)

    most = blocks * width // (rows // chunks)
    sent, now = [0], [0]

    def launch(copy, pieces=1):
        if max(most - n for n in sent) < pieces:
            sent.append(0)
        now[0] = next(n for n, held in enumerate(sent) if held + pieces <= most)
        copy().start()
        sent[now[0]] += pieces

    def all_sent():
        for n, pieces in enumerate(sent):
            pieces, step = (int(pieces), rows // chunks) if pieces == int(pieces) else (int(2 * pieces), rows // chunks // 2)
            over = next(b for b in range(1, blocks + 1) if pieces % b == 0 and pieces // b * step <= width)
            view = lv.at[0:over, 0:pieces // over * step]
            pltpu.make_async_copy(view, view, ref["sent"].at[n]).wait()

    def remote(src, dst, key, k, device):
        return pltpu.make_async_remote_copy(
            src_ref=src, dst_ref=dst,
            send_sem=ref["sent"].at[now[0]], recv_sem=ref[key + ("rcv",)].at[k],
            device_id=device, device_id_type=MESH,
        )

    def to_column(src, dst, key, k, s):
        return remote(src, dst, key, k, {"fsdp": partner(s)})

    def to_group(src, dst, key, k, g):
        return remote(src, dst, key, k, {"grp": g})

    def both_arrived(pair, key, k):
        pltpu.make_async_copy(pair, pair, ref[key + ("rcv",)].at[k]).wait()

    def route_copy(kind, t, way, k):
        f, l = plan[t][way][1:3]
        cand = ref[("cand", t, way, k)]
        if kind == "l":
            return to_column(ref[("sel", t, way, k)], ref[("last", t, way, k)], ("l", t, way), k, l)
        if kind == "p":
            return to_column(ref[("give", t, way, k)], cand.at[side], ("p", t, way), k, 1)
        if kind == "pair":
            return to_column(cand.at[0:2], cand.at[2:4], ("f", t, way), k, f)
        if kind == "e":
            return to_column(ref[("hand", t, way, k)], ref[("take", t, way, k)], ("e", t, way), k, 1)
        if kind == "f":
            return to_column(cand.at[0], cand.at[2], ("f", t, way), k, f)
        if kind == "b":
            return to_column(cand.at[0], cand.at[1], ("b", t, way), k, 1)
        return to_column(cand.at[2], cand.at[3], ("b", t, way), k, 1)

    def enter(t, way, k, piece):
        cand = ref[("cand", t, way, k)]
        if plan[t][way][0] == "H":
            cand[0] = piece
            launch(lambda: route_copy("f", t, way, k))
            launch(lambda: route_copy("b", t, way, k))
        else:
            upper, lower = piece[: rows // 2], piece[rows // 2:]
            cand[side] = jnp.where(side == 0, upper, lower)
            ref[("give", t, way, k)][...] = jnp.where(side == 0, lower, upper)
            launch(lambda: route_copy("p", t, way, k), 0.5)

    def relay(t, way, k):
        if plan[t][way][0] == "H":
            route_copy("f", t, way, k).wait_recv()
            launch(lambda: route_copy("bf", t, way, k))
        else:
            route_copy("p", t, way, k).wait_recv()
            launch(lambda: route_copy("pair", t, way, k))

    def select(t, way, k):
        cand, sel = ref[("cand", t, way, k)], ref[("sel", t, way, k)]
        if plan[t][way][0] == "H":
            both_arrived(cand.at[0:2], ("b", t, way), k)
            sel[...] = cand[plan[t][way][3]]
        else:
            route_copy("pair", t, way, k).wait_recv()
            for n in range(2):
                sel[n] = cand[plan[t][way][3 + n]]
        launch(lambda: route_copy("l", t, way, k))

    def picked(t, way, k, place, last):
        return jnp.where(place == 4, last, ref[("cand", t, way, k)][jnp.minimum(place, 3)])

    def hand_over(t, way, k):
        route_copy("l", t, way, k).wait_recv()
        last = ref[("last", t, way, k)]
        own, other = plan[t][way][5:7]
        ref[("keep", t, way, k)][...] = picked(t, way, k, own, last[side])
        ref[("hand", t, way, k)][...] = picked(t, way, k, other, last[1 - side])
        launch(lambda: route_copy("e", t, way, k), 0.5)

    def leave(t, way, k):
        if plan[t][way][0] == "H":
            route_copy("l", t, way, k).wait_recv()
            return picked(t, way, k, plan[t][way][4], ref[("last", t, way, k)][...])
        route_copy("e", t, way, k).wait_recv()
        keep, take = ref[("keep", t, way, k)][...], ref[("take", t, way, k)][...]
        return jnp.concatenate(
            [jnp.where(side == 0, keep, take), jnp.where(side == 0, take, keep)], axis=0
        )

    def across_copy(t, way, k, g):
        piece = ref[("all", t, way, k)].at[g]
        return to_group(piece, piece, ("across", t, way), k, across)

    def mate_copy(t, way, k, g):
        piece = ref[("all", t, way, k)].at[g]
        return to_group(piece, piece, ("mate", t, way), k, mate)

    def share(t, way, k, piece):
        ref[("all", t, way, k)][grp] = piece
        launch(lambda: across_copy(t, way, k, grp))
        launch(lambda: mate_copy(t, way, k, grp))

    def pass_on(t, way, k):
        across_copy(t, way, k, across).wait_recv()
        launch(lambda: mate_copy(t, way, k, across))

    def gathered(t, way, k):
        both_arrived(ref[("all", t, way, k)].at[0:2], ("mate", t, way), k)

    def whole(t, way, k):
        return ref[("all", t, way, k)][...].reshape(groups * rows, w)

    def dot(a, b):
        return jnp.dot(a, b, preferred_element_type=jnp.float32).astype(out_ref.dtype)

    def home_copy(t, k):
        return to_group(
            ref[("pc", t, "O", k)].at[1 - core], ref[("rcvc", t, "O", k)], ("home", t, "O"), k, mate
        )

    def back_copy(t, k):
        return to_group(
            ref[("sely", t, "O", k)], ref[("rcvy", t, "O", k)], ("back", t, "O"), k, across
        )

    def owner_side(t, k, which):
        return jnp.where(
            owner_core == core, ref[("pc", t, "O", k)][core, which], ref[("rcvc", t, "O", k)][which]
        )

    def offer(t, k, piece_of):
        for g in range(groups):
            ref[("pc", t, "O", k)][g % 2, g // 2] = piece_of(g)
        launch(lambda: home_copy(t, k), 2)

    waited = [False, False, False]

    def loaded(n):
        if not waited[n]:
            loads[n].wait()
            waited[n] = True

    def run(name, t, k):
        q = k % chunks
        slot = plan[t]["slot"]
        if name in ("I0", "G0"):
            loaded(0)
            piece = gv[plan[t]["j"], :, cols_of(q)]
            if name == "I0":
                enter(t, "I", k, piece)
            else:
                share(t, "I", k, piece)
        elif name == "I1":
            relay(t, "I", k)
        elif name == "I2":
            select(t, "I", k)
        elif name in ("IX", "OX"):
            hand_over(t, name[0], k)
        elif name == "I3":
            share(t, "I", k, leave(t, "I", k))
        elif name in ("I4", "G1"):
            pass_on(t, "I", k)
        elif name == "G2":
            gathered(t, "I", k)
        elif name == "I5":
            loaded(1)
            gathered(t, "I", k)
            ref[("lp", t)][:, cols_of(q)] = dot(lv[slot], whole(t, "I", k))
        elif name == "R":
            loaded(2)
            product = dot(ref[("lp", t)][...], rv[slot, :, cols_of(q)])
            offer(t, k, lambda g: product[g * rows:(g + 1) * rows])
        elif name == "S0":
            n = 1 if k < chunks else 2
            loaded(n)
            table = lv if k < chunks else rv
            offer(t, k, lambda g: table[slot, g * rows:(g + 1) * rows, cols_of(q)])
        elif name == "H":
            home_copy(t, k).wait_recv()
            ref[("sely", t, "O", k)][...] = owner_side(t, k, 1 - half)
            launch(lambda: back_copy(t, k))
        elif name == "O0":
            back_copy(t, k).wait_recv()
            mine = owner_side(t, k, half)
            enter(t, "O", k, jnp.where(owner_half == half, mine, ref[("rcvy", t, "O", k)][...]))
        elif name == "O1":
            relay(t, "O", k)
        elif name == "O2":
            select(t, "O", k)
        elif name == "O3":
            piece = leave(t, "O", k)
            if teams[t][0] == "G":
                ref[("fin", t)][:, cols_of(q)] = piece
            elif k < chunks:
                ref[("lrow", t)][:, cols_of(q)] = piece
            else:
                share(t, "O", q, piece)
        elif name == "LG":
            for n in range(chunks):
                ref[("lg", t)][:, cols_of(n)] = dot(ref[("lrow", t)][...], whole(t, "I", n))
        elif name == "O4":
            pass_on(t, "O", q)
        elif name == "O5":
            gathered(t, "O", q)
            ref[("fin", t)][:, cols_of(q)] = dot(ref[("lg", t)][...], whole(t, "O", q))

    pl.semaphore_wait(barrier, 5)
    for step in timetable(teams, chunks):
        run(*step)
    for j in range(blocks):
        value = ref[("fin", 0)][...]
        for t in range(1, blocks):
            value = jnp.where(plan[t]["j"] == j, ref[("fin", t)][...], value)
        out_ref[j] = value
    for n in range(3):
        loaded(n)
    all_sent()


def per_device_fused(gradient, left_factor, right_factor, block_owner):
    blocks, rows, width = gradient.shape
    columns = lax.axis_size("fsdp")
    groups = lax.axis_size("grp")
    far, near = columns // 2, columns // 4
    sides = {"far": (far, near), "near": (near, far)}
    teams = tuple(
        (team[0],) + tuple((way[0],) + sides[way[1]] for way in team[1:]) for team in TEAMS
    )
    held = scratch_of(teams, CHUNKS, blocks, columns, groups, rows, width, gradient.dtype)
    return pl.pallas_call(
        functools.partial(
            preconditioner_kernel, teams, CHUNKS, tuple(held), columns, groups, blocks, rows, width
        ),
        out_shape=jax.ShapeDtypeStruct(gradient.shape, gradient.dtype),
        in_specs=[pl.BlockSpec(memory_space=pltpu.SMEM)] + [pl.BlockSpec(memory_space=pl.ANY)] * 3,
        out_specs=pl.BlockSpec(memory_space=pltpu.VMEM),
        scratch_shapes=list(held.values()),
        compiler_params=pltpu.CompilerParams(
            collective_id=0, has_side_effects=True, vmem_limit_bytes=56033280
        ),
    )(block_owner, gradient, left_factor, right_factor)


def per_device_any(gradient, left_factor, right_factor, block_owner):
    blocks = gradient.shape[0]
    columns = lax.axis_size("fsdp")
    fits = (
        blocks == left_factor.shape[0]
        and blocks == len(TEAMS)
        and lax.axis_size("grp") == 4
        and columns == 8
        and gradient.shape[2] % (CHUNKS * 128) == 0
    )
    body = per_device_fused if fits else per_device
    return body(gradient, left_factor, right_factor, block_owner)


def solution(mesh):
    return jax.shard_map(
        per_device_any,
        mesh=mesh,
        in_specs=(
            P("fsdp", "grp", None),
            P(("fsdp", "grp"), None, None),
            P(("fsdp", "grp"), None, None),
            P(),
        ),
        out_specs=P("fsdp", "grp", None),
        check_vma=False,
    )
```

```python
import functools
import math

import jax
import jax.numpy as jnp
from jax import lax
from jax.experimental import pallas as pl
from jax.experimental.pallas import tpu as pltpu
from jax.sharding import PartitionSpec as P

MESH = pl.DeviceIdType.MESH
CHUNKS = 4
COARSE = 2
SENT = 5
VMEM_LIMIT = 66519040
TEAMS = (('G', ('H', 'far'), ('H', 'near')), ('F', ('H', 'far')), ('F', ('H', 'near')))
ROUTE_STEPS = {"H": "0123", "X": "012X3"}
WHEN = {
    ('I0', 0): (0, 1, 2, 3),
    ('S0', 1): (4, 5, 6, 7, 8, 9, 13, 18),
    ('S0', 2): (10, 25, 28, 38, 44, 51, 59, 72),
    ('H', 1): (11, 12, 14, 15, 16, 17, 22, 27),
    ('H', 2): (19, 30, 33, 41, 49, 57, 69, 77),
    ('G0', 1): (20, 21, 23, 24),
    ('I1', 0): (26, 32, 34, 39),
    ('O0', 1): (29, 31, 35, 37, 40, 42, 53, 67),
    ('I2', 0): (36, 43, 47, 61),
    ('I3', 0): (45, 52, 65, 75),
    ('O0', 2): (46, 64, 74, 81, 89, 94, 100, 106),
    ('O1', 1): (48, 56, 62, 70, 76, 78, 86, 95),
    ('G1', 1): (50, 54, 60, 63),
    ('G2', 1): (55, 58, 68, 73),
    ('O1', 2): (66, 93, 97, 102, 109, 116, 123, 130),
    ('O2', 1): (71, 80, 85, 96, 103, 108, 120, 128),
    ('I4', 0): (79, 87, 99, 105),
    ('G0', 2): (82, 83, 84, 91),
    ('O3', 1): (88, 101, 107, 118, 125, 135, 137, 144),
    ('O2', 2): (90, 119, 131, 138, 143, 147, 152, 154),
    ('I5', 0): (92, 98, 104, 111),
    ('G1', 2): (110, 112, 115, 117),
    ('O3', 2): (113, 141, 151, 156, 163, 167, 170, 172),
    ('R', 0): (114, 121, 126, 132),
    ('LG', 1): (122,),
    ('H', 0): (124, 129, 134, 139),
    ('G2', 2): (127, 133, 136, 146),
    ('O0', 0): (140, 145, 150, 159),
    ('O4', 1): (142, 148, 157, 161),
    ('O5', 1): (149, 155, 162, 165),
    ('O1', 0): (153, 160, 164, 168),
    ('LG', 2): (158,),
    ('O2', 0): (166, 169, 173, 174),
    ('O4', 2): (171, 176, 179, 180),
    ('O5', 2): (175, 178, 182, 183),
    ('O3', 0): (177, 181, 184, 185),
}


def per_device(gradient, left_factor, right_factor, block_owner):
    local_blocks = gradient.shape[0]
    piece_rows = gradient.shape[1]
    block_width = gradient.shape[2]
    slot_count = left_factor.shape[0]
    columns = lax.axis_size("fsdp")
    groups = lax.axis_size("grp")
    column = lax.axis_index("fsdp")
    owners_all = block_owner.reshape(columns, local_blocks)
    dest_column = owners_all // groups
    dest_group = owners_all % groups
    mine_column = lax.dynamic_index_in_dim(dest_column, column, 0, keepdims=False)
    column_ids = jnp.arange(columns, dtype=jnp.int32)
    matching = mine_column[None, :] == column_ids[:, None]
    pick_send = matching.astype(jnp.bfloat16)
    outgoing = jnp.einsum(
        "cj,jrd->crd", pick_send, gradient, preferred_element_type=jnp.float32
    ).astype(jnp.bfloat16)
    arrived = lax.all_to_all(
        outgoing.reshape(columns * piece_rows, block_width),
        "fsdp",
        split_axis=0,
        concat_axis=0,
        tiled=True,
    )
    arrived = arrived.reshape(columns, piece_rows, block_width)
    toward = dest_column == column
    live_source = jnp.sum(toward.astype(jnp.int32), axis=1) > 0
    target = jnp.sum(jnp.where(toward, dest_group, 0), axis=1)
    same_owner = (target[None, :] == target[:, None]) & live_source[None, :] & live_source[:, None]
    before = column_ids[None, :] < column_ids[:, None]
    rank_slot = jnp.sum((same_owner & before).astype(jnp.int32), axis=1)
    group_ids = jnp.arange(groups, dtype=jnp.int32)
    slot_ids = jnp.arange(slot_count, dtype=jnp.int32)
    routing = (
        live_source[None, None, :]
        & (target[None, None, :] == group_ids[:, None, None])
        & (rank_slot[None, None, :] == slot_ids[None, :, None])
    )
    routing = routing.astype(jnp.bfloat16)
    packed = jnp.einsum(
        "oks,srd->kord", routing, arrived, preferred_element_type=jnp.float32
    ).astype(jnp.bfloat16)
    packed = packed.reshape(slot_count, groups * piece_rows, block_width)
    blocks = lax.all_to_all(packed, "grp", split_axis=1, concat_axis=1, tiled=True)
    left_product = jnp.einsum(
        "kab,kbc->kac", left_factor, blocks, preferred_element_type=jnp.float32
    ).astype(jnp.bfloat16)
    result = jnp.einsum(
        "kab,kbc->kac", left_product, right_factor, preferred_element_type=jnp.float32
    ).astype(jnp.bfloat16)
    returned = lax.all_to_all(result, "grp", split_axis=1, concat_axis=1, tiled=True)
    returned = returned.reshape(slot_count, groups, piece_rows, block_width)
    unpacked = jnp.einsum(
        "oks,kord->srd", routing, returned, preferred_element_type=jnp.float32
    ).astype(jnp.bfloat16)
    homeward = lax.all_to_all(
        unpacked.reshape(columns * piece_rows, block_width),
        "fsdp",
        split_axis=0,
        concat_axis=0,
        tiled=True,
    )
    homeward = homeward.reshape(columns, piece_rows, block_width)
    return jnp.einsum(
        "cj,crd->jrd", pick_send, homeward, preferred_element_type=jnp.float32
    ).astype(jnp.bfloat16)


def stages_of(team, chunks):
    if team[0] == "G":
        steps = [w + n for w, way in zip("IO", team[1:]) for n in ROUTE_STEPS[way[0]]]
        return [(name, chunks) for name in steps + ["I4", "I5", "R", "H"]]
    steps = ["S0", "H"] + ["O" + n for n in ROUTE_STEPS[team[1][0]]]
    found = [(name, chunks) for name in ("G0", "G1", "G2", "O4", "O5")]
    return found + [(name, 2 * chunks) for name in steps] + [("LG", 1)]


def timetable(teams, chunks):
    steps = []
    for t, team in enumerate(teams):
        for name, count in stages_of(team, chunks):
            first = chunks if name in ("O4", "O5") else 0
            for i in range(count):
                steps.append((WHEN[(name, t)][i], len(steps), name, t, first + i))
    return [step[2:] for step in sorted(steps)]


def scratch_of(teams, chunks, blocks, columns, groups, rows, width, dtype):
    w = width // chunks
    vmem = lambda *shape: pltpu.VMEM(shape, dtype)
    dma = pltpu.SemaphoreType.DMA
    held = {
        "gv": vmem(blocks, rows, width),
        "lv": vmem(blocks, width, width),
        "rv": vmem(blocks, width, width),
        "load": dma((4,)),
        "owner": pltpu.SMEM((columns * blocks,), jnp.int32),
        "sent": dma((SENT,)),
        "power": pltpu.SMEM((columns,), jnp.int32),
    }

    def copies(key, count):
        held[key + ("rcv",)] = dma((count,))

    def route(key, count, kind):
        for k in range(count):
            if kind == "H":
                held[("cand",) + key + (k,)] = vmem(4, rows, w)
                held[("last",) + key + (k,)] = vmem(rows, w)
                held[("sel",) + key + (k,)] = vmem(rows, w)
            else:
                held[("cand",) + key + (k,)] = vmem(4, rows // 2, w)
                held[("last",) + key + (k,)] = vmem(2, rows // 2, w)
                held[("sel",) + key + (k,)] = vmem(2, rows // 2, w)
                for name in ("give", "keep", "hand", "take"):
                    held[(name,) + key + (k,)] = vmem(rows // 2, w)
        for name in ("f", "b", "l") if kind == "H" else ("p", "f", "l", "e"):
            copies((name,) + key, count)

    def gather(key, count):
        for k in range(count):
            held[("all",) + key + (k,)] = vmem(groups, rows, w)
        for name in ("across", "mate"):
            copies((name,) + key, count)

    def scatter(key, count):
        for k in range(count):
            held[("pc",) + key + (k,)] = vmem(2, 2, rows, w)
            held[("rcvc",) + key + (k,)] = vmem(2, rows, w)
            held[("sely",) + key + (k,)] = vmem(rows, w)
            held[("rcvy",) + key + (k,)] = vmem(rows, w)
        for name in ("home", "back"):
            copies((name,) + key, count)

    for t, team in enumerate(teams):
        held[("fin", t)] = vmem(rows, width)
        if team[0] == "G":
            route((t, "I"), chunks, team[1][0])
            gather((t, "I"), chunks)
            held[("lp", t)] = vmem(width, width)
            scatter((t, "O"), chunks)
            route((t, "O"), chunks, team[2][0])
        else:
            gather((t, "I"), chunks)
            scatter((t, "O"), 2 * chunks)
            route((t, "O"), 2 * chunks, team[1][0])
            gather((t, "O"), chunks)
            held[("lrow", t)] = vmem(rows, width)
            held[("lg", t)] = vmem(rows, width)
    return held


def preconditioner_kernel(
    teams, chunks, names, columns, groups, blocks, rows, width,
    owner_hbm, g_hbm, l_hbm, r_hbm, out_ref, *rest,
):
    ref = dict(zip(names, rest))
    col = lax.axis_index("fsdp")
    grp = lax.axis_index("grp")
    core = grp % 2
    half = grp // 2
    mate = half * 2 + (1 - core)
    across = (1 - half) * 2 + core
    w = width // chunks
    zero = jnp.int32(0)

    def cols_of(q):
        return slice(q * w, (q + 1) * w)

    def partner(s):
        d, b = 0, 1
        while b < columns:
            v = (col // b) % 2
            d, b = d + b * ((1 - v) if s & b else v), 2 * b
        return d

    gv, lv, rv, owner_ref = ref["gv"], ref["lv"], ref["rv"], ref["owner"]
    loads = [
        pltpu.make_async_copy(g_hbm, gv, ref["load"].at[0]),
        pltpu.make_async_copy(l_hbm, lv, ref["load"].at[1]),
        pltpu.make_async_copy(r_hbm, rv, ref["load"].at[2]),
        pltpu.make_async_copy(owner_hbm, owner_ref, ref["load"].at[3]),
    ]
    for load in loads[::-1]:
        load.start()

    far, near = columns // 2, columns // 4
    barrier = pltpu.get_barrier_semaphore()
    for s in (1, near, far):
        pl.semaphore_signal(barrier, inc=1, device_id={"fsdp": partner(s)}, device_id_type=MESH)
    for g in (mate, across):
        pl.semaphore_signal(barrier, inc=1, device_id={"grp": g}, device_id_type=MESH)

    def look_up(table, index):
        found = zero
        for n, value in enumerate(table):
            found = jnp.where(index == n, value, found)
        return found

    loads[3].wait()
    power = ref["power"]
    for d in range(columns):
        power[d] = jnp.int32(2 ** d)
    to = [[owner_ref[c * blocks + j] // groups for j in range(blocks)] for c in range(columns)]
    left_over = [[(jnp.int32(j), to[c][j], power[to[c][j]]) for j in range(blocks)] for c in range(columns)]
    pick, dest = [], []
    full = 2 ** columns - 1
    while len(left_over[0]) > 1:
        m = len(left_over[0])
        count = m ** columns
        tall = -(-count // 1024) * 8
        inverse = -(-(2 ** 17) // m)
        index = (
            lax.broadcasted_iota(jnp.int32, (tall, 128), 0) * 128
            + lax.broadcasted_iota(jnp.int32, (tall, 128), 1)
        )
        rest_of, reach = index, jnp.zeros((tall, 128), jnp.int32)
        for c in range(columns):
            upper = (rest_of * inverse) >> 17
            digit = rest_of - upper * m
            bit = jnp.full((tall, 128), left_over[c][m - 1][2], jnp.int32)
            for i in range(m - 1):
                bit = jnp.where(digit == i, left_over[c][i][2], bit)
            reach, rest_of = reach | bit, upper
        chosen = jnp.min(jnp.where((reach == full) & (index < count), index, count - 1))
        pick_t, dest_t = [], []
        for c in range(columns):
            upper = (chosen * inverse) >> 17
            digit, chosen = chosen - upper * m, upper
            pick_t.append(look_up([e[0] for e in left_over[c]], digit))
            dest_t.append(look_up([e[1] for e in left_over[c]], digit))
            left_over[c] = [
                tuple(jnp.where(digit <= i, b, a) for a, b in zip(left_over[c][i], left_over[c][i + 1]))
                for i in range(m - 1)
            ]
        pick.append(pick_t)
        dest.append(dest_t)
    pick.append([left_over[c][0][0] for c in range(columns)])
    dest.append([left_over[c][0][1] for c in range(columns)])

    owner_group = zero
    for c in range(columns):
        for j in range(blocks):
            owner_group = jnp.where(to[c][j] == col, owner_ref[c * blocks + j] % groups, owner_group)
    owner_core = owner_group % 2
    owner_half = owner_group // 2
    reaches = []
    for c in range(columns):
        hit = zero
        for j in range(blocks):
            hit = jnp.where(to[c][j] == col, 1, hit)
        reaches.append(hit)

    def source_of(t, d):
        found = zero
        for c in range(columns):
            found = jnp.where(dest[t][c] == d, c, found)
        return found

    def place_among(wanted, f, other):
        found = jnp.int32(other)
        for n, s in enumerate((0, 1, f, f + 1)):
            found = jnp.where(wanted == partner(s), n, found)
        return found

    side = col % 2

    def route_plan(way, origin):
        kind, f, l = way
        if kind == "H":
            return kind, f, l, place_among(origin(partner(l)), f, 0), place_among(origin(col), f, 4)
        there = partner(l) - side
        held_by = (col - side, col - side + 1, partner(f) - side, partner(f) - side + 1)

        def place(d, other):
            found, wanted = jnp.int32(other), origin(d)
            for n, c in enumerate(held_by):
                found = jnp.where(wanted == c, n, found)
            return found

        return kind, f, l, place(there, 0), place(there + 1, 0), place(col, 4), place(partner(1), 4)

    plan = []
    for t, team in enumerate(teams):
        mine = {"j": look_up(pick[t], col)}
        src = source_of(t, col)
        slot = zero
        for c in range(columns):
            slot = slot + jnp.where(c < src, reaches[c], 0)
        mine["slot"] = jnp.minimum(slot, blocks - 1)
        if team[0] == "G":
            mine["I"] = route_plan(team[1], functools.partial(source_of, t))
        mine["O"] = route_plan(team[-1], functools.partial(look_up, dest[t]))
        plan.append(mine)

    most = blocks * width // (rows // chunks)
    sent, now = [0], [0]

    def launch(copy, pieces=1):
        if max(most - n for n in sent) < pieces:
            sent.append(0)
        now[0] = next(n for n, held in enumerate(sent) if held + pieces <= most)
        copy().start()
        sent[now[0]] += pieces

    def all_sent():
        for n, pieces in enumerate(sent):
            pieces, step = (int(pieces), rows // chunks) if pieces == int(pieces) else (int(2 * pieces), rows // chunks // 2)
            over = next(b for b in range(1, blocks + 1) if pieces % b == 0 and pieces // b * step <= width)
            view = lv.at[0:over, 0:pieces // over * step]
            pltpu.make_async_copy(view, view, ref["sent"].at[n]).wait()

    def remote(src, dst, key, k, device):
        return pltpu.make_async_remote_copy(
            src_ref=src, dst_ref=dst,
            send_sem=ref["sent"].at[now[0]], recv_sem=ref[key + ("rcv",)].at[k],
            device_id=device, device_id_type=MESH,
        )

    def to_column(src, dst, key, k, s):
        return remote(src, dst, key, k, {"fsdp": partner(s)})

    def to_group(src, dst, key, k, g):
        return remote(src, dst, key, k, {"grp": g})

    def both_arrived(pair, key, k):
        pltpu.make_async_copy(pair, pair, ref[key + ("rcv",)].at[k]).wait()

    def route_copy(kind, t, way, k):
        f, l = plan[t][way][1:3]
        cand = ref[("cand", t, way, k)]
        if kind == "l":
            return to_column(ref[("sel", t, way, k)], ref[("last", t, way, k)], ("l", t, way), k, l)
        if kind == "p":
            return to_column(ref[("give", t, way, k)], cand.at[side], ("p", t, way), k, 1)
        if kind == "pair":
            return to_column(cand.at[0:2], cand.at[2:4], ("f", t, way), k, f)
        if kind == "e":
            return to_column(ref[("hand", t, way, k)], ref[("take", t, way, k)], ("e", t, way), k, 1)
        if kind == "f":
            return to_column(cand.at[0], cand.at[2], ("f", t, way), k, f)
        if kind == "b":
            return to_column(cand.at[0], cand.at[1], ("b", t, way), k, 1)
        return to_column(cand.at[2], cand.at[3], ("b", t, way), k, 1)

    def enter(t, way, k, piece):
        cand = ref[("cand", t, way, k)]
        if plan[t][way][0] == "H":
            cand[0] = piece
            launch(lambda: route_copy("f", t, way, k))
            launch(lambda: route_copy("b", t, way, k))
        else:
            upper, lower = piece[: rows // 2], piece[rows // 2:]
            cand[side] = jnp.where(side == 0, upper, lower)
            ref[("give", t, way, k)][...] = jnp.where(side == 0, lower, upper)
            launch(lambda: route_copy("p", t, way, k), 0.5)

    def relay(t, way, k):
        if plan[t][way][0] == "H":
            route_copy("f", t, way, k).wait_recv()
            launch(lambda: route_copy("bf", t, way, k))
        else:
            route_copy("p", t, way, k).wait_recv()
            launch(lambda: route_copy("pair", t, way, k))

    def select(t, way, k):
        cand, sel = ref[("cand", t, way, k)], ref[("sel", t, way, k)]
        if plan[t][way][0] == "H":
            both_arrived(cand.at[0:2], ("b", t, way), k)
            sel[...] = cand[plan[t][way][3]]
        else:
            route_copy("pair", t, way, k).wait_recv()
            for n in range(2):
                sel[n] = cand[plan[t][way][3 + n]]
        launch(lambda: route_copy("l", t, way, k))

    def picked(t, way, k, place, last):
        return jnp.where(place == 4, last, ref[("cand", t, way, k)][jnp.minimum(place, 3)])

    def hand_over(t, way, k):
        route_copy("l", t, way, k).wait_recv()
        last = ref[("last", t, way, k)]
        own, other = plan[t][way][5:7]
        ref[("keep", t, way, k)][...] = picked(t, way, k, own, last[side])
        ref[("hand", t, way, k)][...] = picked(t, way, k, other, last[1 - side])
        launch(lambda: route_copy("e", t, way, k), 0.5)

    def leave(t, way, k):
        if plan[t][way][0] == "H":
            route_copy("l", t, way, k).wait_recv()
            return picked(t, way, k, plan[t][way][4], ref[("last", t, way, k)][...])
        route_copy("e", t, way, k).wait_recv()
        keep, take = ref[("keep", t, way, k)][...], ref[("take", t, way, k)][...]
        return jnp.concatenate(
            [jnp.where(side == 0, keep, take), jnp.where(side == 0, take, keep)], axis=0
        )

    def across_copy(t, way, k, g):
        piece = ref[("all", t, way, k)].at[g]
        return to_group(piece, piece, ("across", t, way), k, across)

    def mate_copy(t, way, k, g):
        piece = ref[("all", t, way, k)].at[g]
        return to_group(piece, piece, ("mate", t, way), k, mate)

    def share(t, way, k, piece):
        ref[("all", t, way, k)][grp] = piece
        launch(lambda: across_copy(t, way, k, grp))
        launch(lambda: mate_copy(t, way, k, grp))

    def pass_on(t, way, k):
        across_copy(t, way, k, across).wait_recv()
        launch(lambda: mate_copy(t, way, k, across))

    def gathered(t, way, k):
        both_arrived(ref[("all", t, way, k)].at[0:2], ("mate", t, way), k)

    def whole(t, way, k):
        return ref[("all", t, way, k)][...].reshape(groups * rows, w)

    def dot(a, b):
        return jnp.dot(a, b, preferred_element_type=jnp.float32).astype(out_ref.dtype)

    def home_copy(t, k):
        return to_group(
            ref[("pc", t, "O", k)].at[1 - core], ref[("rcvc", t, "O", k)], ("home", t, "O"), k, mate
        )

    def back_copy(t, k):
        return to_group(
            ref[("sely", t, "O", k)], ref[("rcvy", t, "O", k)], ("back", t, "O"), k, across
        )

    def owner_side(t, k, which):
        return jnp.where(
            owner_core == core, ref[("pc", t, "O", k)][core, which], ref[("rcvc", t, "O", k)][which]
        )

    def offer(t, k, piece_of):
        for g in range(groups):
            ref[("pc", t, "O", k)][g % 2, g // 2] = piece_of(g)
        launch(lambda: home_copy(t, k), 2)

    waited = [False, False, False]

    def loaded(n):
        if not waited[n]:
            loads[n].wait()
            waited[n] = True

    def run(name, t, k):
        q = k % chunks
        slot = plan[t]["slot"]
        if name in ("I0", "G0"):
            loaded(0)
            piece = gv[plan[t]["j"], :, cols_of(q)]
            if name == "I0":
                enter(t, "I", k, piece)
            else:
                share(t, "I", k, piece)
        elif name == "I1":
            relay(t, "I", k)
        elif name == "I2":
            select(t, "I", k)
        elif name in ("IX", "OX"):
            hand_over(t, name[0], k)
        elif name == "I3":
            share(t, "I", k, leave(t, "I", k))
        elif name in ("I4", "G1"):
            pass_on(t, "I", k)
        elif name == "G2":
            gathered(t, "I", k)
        elif name == "I5":
            loaded(1)
            gathered(t, "I", k)
            ref[("lp", t)][:, cols_of(q)] = dot(lv[slot], whole(t, "I", k))
        elif name == "R":
            loaded(2)
            product = dot(ref[("lp", t)][...], rv[slot, :, cols_of(q)])
            offer(t, k, lambda g: product[g * rows:(g + 1) * rows])
        elif name == "S0":
            n = 1 if k < chunks else 2
            loaded(n)
            table = lv if k < chunks else rv
            offer(t, k, lambda g: table[slot, g * rows:(g + 1) * rows, cols_of(q)])
        elif name == "H":
            home_copy(t, k).wait_recv()
            ref[("sely", t, "O", k)][...] = owner_side(t, k, 1 - half)
            launch(lambda: back_copy(t, k))
        elif name == "O0":
            back_copy(t, k).wait_recv()
            mine = owner_side(t, k, half)
            enter(t, "O", k, jnp.where(owner_half == half, mine, ref[("rcvy", t, "O", k)][...]))
        elif name == "O1":
            relay(t, "O", k)
        elif name == "O2":
            select(t, "O", k)
        elif name == "O3":
            piece = leave(t, "O", k)
            if teams[t][0] == "G":
                ref[("fin", t)][:, cols_of(q)] = piece
            elif k < chunks:
                ref[("lrow", t)][:, cols_of(q)] = piece
            else:
                share(t, "O", q, piece)
        elif name == "LG":
            for n in range(chunks):
                ref[("lg", t)][:, cols_of(n)] = dot(ref[("lrow", t)][...], whole(t, "I", n))
        elif name == "O4":
            pass_on(t, "O", q)
        elif name == "O5":
            gathered(t, "O", q)
            ref[("fin", t)][:, cols_of(q)] = dot(ref[("lg", t)][...], whole(t, "O", q))

    pl.semaphore_wait(barrier, 5)
    for step in timetable(teams, chunks):
        run(*step)
    for j in range(blocks):
        value = ref[("fin", 0)][...]
        for t in range(1, blocks):
            value = jnp.where(plan[t]["j"] == j, ref[("fin", t)][...], value)
        out_ref[j] = value
    for n in range(3):
        loaded(n)
    all_sent()


def per_device_fused(gradient, left_factor, right_factor, block_owner):
    blocks, rows, width = gradient.shape
    columns = lax.axis_size("fsdp")
    groups = lax.axis_size("grp")
    far, near = columns // 2, columns // 4
    sides = {"far": (far, near), "near": (near, far)}
    teams = tuple(
        (team[0],) + tuple((way[0],) + sides[way[1]] for way in team[1:]) for team in TEAMS
    )
    held = scratch_of(teams, CHUNKS, blocks, columns, groups, rows, width, gradient.dtype)
    return pl.pallas_call(
        functools.partial(
            preconditioner_kernel, teams, CHUNKS, tuple(held), columns, groups, blocks, rows, width
        ),
        out_shape=pltpu.VMEM(gradient.shape, gradient.dtype),
        in_specs=[pl.BlockSpec(memory_space=pl.ANY)] * 4,
        out_specs=pl.BlockSpec(memory_space=pltpu.VMEM),
        scratch_shapes=list(held.values()),
        compiler_params=pltpu.CompilerParams(
            collective_id=0, has_side_effects=True, vmem_limit_bytes=VMEM_LIMIT
        ),
    )(block_owner, gradient, left_factor, right_factor)


def per_device_any(gradient, left_factor, right_factor, block_owner):
    blocks = gradient.shape[0]
    columns = lax.axis_size("fsdp")
    fits = (
        blocks == left_factor.shape[0]
        and blocks == len(TEAMS)
        and lax.axis_size("grp") == 4
        and columns == 8
        and gradient.shape[2] % (CHUNKS * 128) == 0
    )
    body = per_device_fused if fits else per_device
    return body(gradient, left_factor, right_factor, block_owner)


def solution(mesh):
    return jax.shard_map(
        per_device_any,
        mesh=mesh,
        in_specs=(
            P("fsdp", "grp", None),
            P(("fsdp", "grp"), None, None),
            P(("fsdp", "grp"), None, None),
            P(),
        ),
        out_specs=P("fsdp", "grp", None),
        check_vma=False,
    )
```

```python
import functools
import math

import jax
import jax.numpy as jnp
from jax import lax
from jax.experimental import pallas as pl
from jax.experimental.pallas import tpu as pltpu
from jax.sharding import PartitionSpec as P

MESH = pl.DeviceIdType.MESH
CHUNKS = 4
COARSE = 2
SENT = 5
DIRECT = ((0, "I"),)
VMEM_LIMIT = 66519040
TEAMS = (('G', ('H', 'far'), ('H', 'near')), ('F', ('H', 'far')), ('F', ('H', 'near')))
ROUTE_STEPS = {"H": "0123", "X": "012X3"}
WHEN = {
    ('I0', 0): (0, 1, 2, 3),
    ('S0', 2): (4, 20, 23, 36, 43, 49, 58, 69),
    ('S0', 1): (5, 6, 7, 8, 9, 10, 14, 19),
    ('H', 2): (11, 26, 31, 40, 48, 53, 67, 76),
    ('H', 1): (12, 13, 15, 16, 17, 18, 22, 27),
    ('I1', 0): (21, 30, 33, 37),
    ('G0', 1): (24, 25, 28, 29),
    ('O0', 1): (32, 34, 38, 39, 41, 44, 54, 68),
    ('I2', 0): (35, 42, 47, 59),
    ('I3', 0): (45, 52, 61, 74),
    ('O0', 2): (46, 60, 70, 78, 86, 93, 98, 105),
    ('O1', 1): (50, 57, 65, 72, 83, 84, 90, 99),
    ('G1', 1): (51, 55, 64, 66),
    ('G2', 1): (56, 63, 71, 75),
    ('O1', 2): (62, 92, 95, 100, 107, 116, 120, 127),
    ('O2', 1): (73, 85, 88, 101, 106, 109, 123, 131),
    ('I4', 0): (77, 80, 97, 104),
    ('G0', 2): (79, 81, 82, 89),
    ('O2', 2): (87, 118, 128, 134, 142, 144, 150, 152),
    ('I5', 0): (91, 96, 103, 111),
    ('O3', 1): (94, 102, 108, 121, 130, 137, 139, 146),
    ('G1', 2): (110, 112, 115, 117),
    ('O3', 2): (113, 141, 149, 155, 161, 165, 170, 172),
    ('R', 0): (114, 119, 124, 129),
    ('H', 0): (122, 126, 133, 136),
    ('LG', 1): (125,),
    ('G2', 2): (132, 135, 138, 147),
    ('O0', 0): (140, 143, 148, 157),
    ('O4', 1): (145, 153, 160, 162),
    ('O1', 0): (151, 158, 163, 168),
    ('O5', 1): (154, 159, 166, 167),
    ('LG', 2): (156,),
    ('O2', 0): (164, 169, 173, 174),
    ('O4', 2): (171, 176, 179, 180),
    ('O5', 2): (175, 178, 182, 183),
    ('O3', 0): (177, 181, 184, 185),
}


def per_device(gradient, left_factor, right_factor, block_owner):
    local_blocks = gradient.shape[0]
    piece_rows = gradient.shape[1]
    block_width = gradient.shape[2]
    slot_count = left_factor.shape[0]
    columns = lax.axis_size("fsdp")
    groups = lax.axis_size("grp")
    column = lax.axis_index("fsdp")
    owners_all = block_owner.reshape(columns, local_blocks)
    dest_column = owners_all // groups
    dest_group = owners_all % groups
    mine_column = lax.dynamic_index_in_dim(dest_column, column, 0, keepdims=False)
    column_ids = jnp.arange(columns, dtype=jnp.int32)
    matching = mine_column[None, :] == column_ids[:, None]
    pick_send = matching.astype(jnp.bfloat16)
    outgoing = jnp.einsum(
        "cj,jrd->crd", pick_send, gradient, preferred_element_type=jnp.float32
    ).astype(jnp.bfloat16)
    arrived = lax.all_to_all(
        outgoing.reshape(columns * piece_rows, block_width),
        "fsdp",
        split_axis=0,
        concat_axis=0,
        tiled=True,
    )
    arrived = arrived.reshape(columns, piece_rows, block_width)
    toward = dest_column == column
    live_source = jnp.sum(toward.astype(jnp.int32), axis=1) > 0
    target = jnp.sum(jnp.where(toward, dest_group, 0), axis=1)
    same_owner = (target[None, :] == target[:, None]) & live_source[None, :] & live_source[:, None]
    before = column_ids[None, :] < column_ids[:, None]
    rank_slot = jnp.sum((same_owner & before).astype(jnp.int32), axis=1)
    group_ids = jnp.arange(groups, dtype=jnp.int32)
    slot_ids = jnp.arange(slot_count, dtype=jnp.int32)
    routing = (
        live_source[None, None, :]
        & (target[None, None, :] == group_ids[:, None, None])
        & (rank_slot[None, None, :] == slot_ids[None, :, None])
    )
    routing = routing.astype(jnp.bfloat16)
    packed = jnp.einsum(
        "oks,srd->kord", routing, arrived, preferred_element_type=jnp.float32
    ).astype(jnp.bfloat16)
    packed = packed.reshape(slot_count, groups * piece_rows, block_width)
    blocks = lax.all_to_all(packed, "grp", split_axis=1, concat_axis=1, tiled=True)
    left_product = jnp.einsum(
        "kab,kbc->kac", left_factor, blocks, preferred_element_type=jnp.float32
    ).astype(jnp.bfloat16)
    result = jnp.einsum(
        "kab,kbc->kac", left_product, right_factor, preferred_element_type=jnp.float32
    ).astype(jnp.bfloat16)
    returned = lax.all_to_all(result, "grp", split_axis=1, concat_axis=1, tiled=True)
    returned = returned.reshape(slot_count, groups, piece_rows, block_width)
    unpacked = jnp.einsum(
        "oks,kord->srd", routing, returned, preferred_element_type=jnp.float32
    ).astype(jnp.bfloat16)
    homeward = lax.all_to_all(
        unpacked.reshape(columns * piece_rows, block_width),
        "fsdp",
        split_axis=0,
        concat_axis=0,
        tiled=True,
    )
    homeward = homeward.reshape(columns, piece_rows, block_width)
    return jnp.einsum(
        "cj,crd->jrd", pick_send, homeward, preferred_element_type=jnp.float32
    ).astype(jnp.bfloat16)


def stages_of(team, chunks):
    if team[0] == "G":
        steps = [w + n for w, way in zip("IO", team[1:]) for n in ROUTE_STEPS[way[0]]]
        return [(name, chunks) for name in steps + ["I4", "I5", "R", "H"]]
    steps = ["S0", "H"] + ["O" + n for n in ROUTE_STEPS[team[1][0]]]
    found = [(name, chunks) for name in ("G0", "G1", "G2", "O4", "O5")]
    return found + [(name, 2 * chunks) for name in steps] + [("LG", 1)]


def timetable(teams, chunks):
    steps = []
    for t, team in enumerate(teams):
        for name, count in stages_of(team, chunks):
            first = chunks if name in ("O4", "O5") else 0
            for i in range(count):
                steps.append((WHEN[(name, t)][i], len(steps), name, t, first + i))
    return [step[2:] for step in sorted(steps)]


def scratch_of(teams, chunks, blocks, columns, groups, rows, width, dtype):
    w = width // chunks
    vmem = lambda *shape: pltpu.VMEM(shape, dtype)
    dma = pltpu.SemaphoreType.DMA
    held = {
        "gv": vmem(blocks, rows, width),
        "lv": vmem(blocks, width, width),
        "rv": vmem(blocks, width, width),
        "load": dma((4,)),
        "owner": pltpu.SMEM((columns * blocks,), jnp.int32),
        "sent": dma((SENT,)),
        "power": pltpu.SMEM((columns,), jnp.int32),
    }

    def copies(key, count):
        held[key + ("rcv",)] = dma((count,))

    def route(key, count, kind):
        for k in range(count):
            if kind == "H":
                held[("cand",) + key + (k,)] = vmem(4, rows, w)
                held[("last",) + key + (k,)] = vmem(rows, w)
                held[("sel",) + key + (k,)] = vmem(rows, w)
            else:
                held[("cand",) + key + (k,)] = vmem(4, rows // 2, w)
                held[("last",) + key + (k,)] = vmem(2, rows // 2, w)
                held[("sel",) + key + (k,)] = vmem(2, rows // 2, w)
                for name in ("give", "keep", "hand", "take"):
                    held[(name,) + key + (k,)] = vmem(rows // 2, w)
        for name in ("f", "b", "l") if kind == "H" else ("p", "f", "l", "e"):
            copies((name,) + key, count)
        if count > chunks:
            copies(("l",) + key, 1 + count - chunks)

    def gather(key, count, waits):
        for k in range(count):
            held[("all",) + key + (k,)] = vmem(groups, rows, w)
        for name in ("across", "mate"):
            copies((name,) + key, waits)

    def scatter(key, count):
        for k in range(count):
            held[("pc",) + key + (k,)] = vmem(2, 2, rows, w)
            held[("rcvc",) + key + (k,)] = vmem(2, rows, w)
            held[("sely",) + key + (k,)] = vmem(rows, w)
            held[("rcvy",) + key + (k,)] = vmem(rows, w)
        for name in ("home", "back"):
            copies((name,) + key, count)

    for t, team in enumerate(teams):
        held[("fin", t)] = vmem(rows, width)
        if team[0] == "G":
            route((t, "I"), chunks, team[1][0])
            gather((t, "I"), chunks, chunks)
            held[("lp", t)] = vmem(width, width)
            scatter((t, "O"), chunks)
            route((t, "O"), chunks, team[2][0])
        else:
            gather((t, "I"), chunks, 1)
            scatter((t, "O"), 2 * chunks)
            route((t, "O"), 2 * chunks, team[1][0])
            gather((t, "O"), chunks, chunks)
            held[("lrow", t)] = vmem(rows, width)
            held[("lg", t)] = vmem(rows, width)
    return held


def preconditioner_kernel(
    teams, chunks, names, columns, groups, blocks, rows, width,
    owner_hbm, g_hbm, l_hbm, r_hbm, out_ref, *rest,
):
    ref = dict(zip(names, rest))
    col = lax.axis_index("fsdp")
    grp = lax.axis_index("grp")
    core = grp % 2
    half = grp // 2
    mate = half * 2 + (1 - core)
    across = (1 - half) * 2 + core
    diagonal = (1 - half) * 2 + (1 - core)
    w = width // chunks
    zero = jnp.int32(0)

    def cols_of(q):
        return slice(q * w, (q + 1) * w)

    def partner(s):
        d, b = 0, 1
        while b < columns:
            v = (col // b) % 2
            d, b = d + b * ((1 - v) if s & b else v), 2 * b
        return d

    gv, lv, rv, owner_ref = ref["gv"], ref["lv"], ref["rv"], ref["owner"]
    loads = [
        pltpu.make_async_copy(g_hbm, gv, ref["load"].at[0]),
        pltpu.make_async_copy(l_hbm, lv, ref["load"].at[1]),
        pltpu.make_async_copy(r_hbm, rv, ref["load"].at[2]),
        pltpu.make_async_copy(owner_hbm, owner_ref, ref["load"].at[3]),
    ]
    for load in loads[::-1]:
        load.start()

    far, near = columns // 2, columns // 4
    barrier = pltpu.get_barrier_semaphore()
    for s in (1, near, far):
        pl.semaphore_signal(barrier, inc=1, device_id={"fsdp": partner(s)}, device_id_type=MESH)
    for g in (mate, across, diagonal):
        pl.semaphore_signal(barrier, inc=1, device_id={"grp": g}, device_id_type=MESH)

    def look_up(table, index):
        found = zero
        for n, value in enumerate(table):
            found = jnp.where(index == n, value, found)
        return found

    loads[3].wait()
    power = ref["power"]
    for d in range(columns):
        power[d] = jnp.int32(2 ** d)
    to = [[owner_ref[c * blocks + j] // groups for j in range(blocks)] for c in range(columns)]
    left_over = [[(jnp.int32(j), to[c][j], power[to[c][j]]) for j in range(blocks)] for c in range(columns)]
    pick, dest = [], []
    full = 2 ** columns - 1
    while len(left_over[0]) > 1:
        m = len(left_over[0])
        count = m ** columns
        tall = -(-count // 1024) * 8
        inverse = -(-(2 ** 17) // m)
        index = (
            lax.broadcasted_iota(jnp.int32, (tall, 128), 0) * 128
            + lax.broadcasted_iota(jnp.int32, (tall, 128), 1)
        )
        rest_of, reach = index, jnp.zeros((tall, 128), jnp.int32)
        for c in range(columns):
            upper = (rest_of * inverse) >> 17
            digit = rest_of - upper * m
            bit = jnp.full((tall, 128), left_over[c][m - 1][2], jnp.int32)
            for i in range(m - 1):
                bit = jnp.where(digit == i, left_over[c][i][2], bit)
            reach, rest_of = reach | bit, upper
        chosen = jnp.min(jnp.where((reach == full) & (index < count), index, count - 1))
        pick_t, dest_t = [], []
        for c in range(columns):
            upper = (chosen * inverse) >> 17
            digit, chosen = chosen - upper * m, upper
            pick_t.append(look_up([e[0] for e in left_over[c]], digit))
            dest_t.append(look_up([e[1] for e in left_over[c]], digit))
            left_over[c] = [
                tuple(jnp.where(digit <= i, b, a) for a, b in zip(left_over[c][i], left_over[c][i + 1]))
                for i in range(m - 1)
            ]
        pick.append(pick_t)
        dest.append(dest_t)
    pick.append([left_over[c][0][0] for c in range(columns)])
    dest.append([left_over[c][0][1] for c in range(columns)])

    owner_group = zero
    for c in range(columns):
        for j in range(blocks):
            owner_group = jnp.where(to[c][j] == col, owner_ref[c * blocks + j] % groups, owner_group)
    owner_core = owner_group % 2
    owner_half = owner_group // 2
    reaches = []
    for c in range(columns):
        hit = zero
        for j in range(blocks):
            hit = jnp.where(to[c][j] == col, 1, hit)
        reaches.append(hit)

    def source_of(t, d):
        found = zero
        for c in range(columns):
            found = jnp.where(dest[t][c] == d, c, found)
        return found

    def place_among(wanted, f, other):
        found = jnp.int32(other)
        for n, s in enumerate((0, 1, f, f + 1)):
            found = jnp.where(wanted == partner(s), n, found)
        return found

    side = col % 2

    def route_plan(way, origin):
        kind, f, l = way
        if kind == "H":
            return kind, f, l, place_among(origin(partner(l)), f, 0), place_among(origin(col), f, 4)
        there = partner(l) - side
        held_by = (col - side, col - side + 1, partner(f) - side, partner(f) - side + 1)

        def place(d, other):
            found, wanted = jnp.int32(other), origin(d)
            for n, c in enumerate(held_by):
                found = jnp.where(wanted == c, n, found)
            return found

        return kind, f, l, place(there, 0), place(there + 1, 0), place(col, 4), place(partner(1), 4)

    plan = []
    for t, team in enumerate(teams):
        mine = {"j": look_up(pick[t], col)}
        src = source_of(t, col)
        slot = zero
        for c in range(columns):
            slot = slot + jnp.where(c < src, reaches[c], 0)
        mine["slot"] = jnp.minimum(slot, blocks - 1)
        if team[0] == "G":
            mine["I"] = route_plan(team[1], functools.partial(source_of, t))
        mine["O"] = route_plan(team[-1], functools.partial(look_up, dest[t]))
        plan.append(mine)

    most = blocks * width // (rows // chunks)
    sent, now = [0], [0]

    def launch(copy, pieces=1):
        if max(most - n for n in sent) < pieces:
            sent.append(0)
        now[0] = next(n for n, held in enumerate(sent) if held + pieces <= most)
        copy().start()
        sent[now[0]] += pieces

    def all_sent():
        for n, pieces in enumerate(sent):
            pieces, step = (int(pieces), rows // chunks) if pieces == int(pieces) else (int(2 * pieces), rows // chunks // 2)
            over = next(b for b in range(1, blocks + 1) if pieces % b == 0 and pieces // b * step <= width)
            view = lv.at[0:over, 0:pieces // over * step]
            pltpu.make_async_copy(view, view, ref["sent"].at[n]).wait()

    def remote(src, dst, key, k, device):
        return pltpu.make_async_remote_copy(
            src_ref=src, dst_ref=dst,
            send_sem=ref["sent"].at[now[0]], recv_sem=ref[key + ("rcv",)].at[k],
            device_id=device, device_id_type=MESH,
        )

    def to_column(src, dst, key, k, s):
        return remote(src, dst, key, k, {"fsdp": partner(s)})

    def to_group(src, dst, key, k, g):
        return remote(src, dst, key, k, {"grp": g})

    def both_arrived(pair, key, k):
        pltpu.make_async_copy(pair, pair, ref[key + ("rcv",)].at[k]).wait()

    def route_copy(kind, t, way, k):
        f, l = plan[t][way][1:3]
        cand = ref[("cand", t, way, k)]
        if kind == "l":
            n = k if teams[t][0] == "G" else max(0, k - chunks + 1)
            return to_column(ref[("sel", t, way, k)], ref[("last", t, way, k)], ("l", t, way), n, l)
        if kind == "p":
            return to_column(ref[("give", t, way, k)], cand.at[side], ("p", t, way), k, 1)
        if kind == "pair":
            return to_column(cand.at[0:2], cand.at[2:4], ("f", t, way), k, f)
        if kind == "e":
            return to_column(ref[("hand", t, way, k)], ref[("take", t, way, k)], ("e", t, way), k, 1)
        if kind == "f":
            return to_column(cand.at[0], cand.at[2], ("f", t, way), k, f)
        if kind == "b":
            return to_column(cand.at[0], cand.at[1], ("b", t, way), k, 1)
        return to_column(cand.at[2], cand.at[3], ("b", t, way), k, 1)

    def enter(t, way, k, piece):
        cand = ref[("cand", t, way, k)]
        if plan[t][way][0] == "H":
            cand[0] = piece
            launch(lambda: route_copy("f", t, way, k))
            launch(lambda: route_copy("b", t, way, k))
        else:
            upper, lower = piece[: rows // 2], piece[rows // 2:]
            cand[side] = jnp.where(side == 0, upper, lower)
            ref[("give", t, way, k)][...] = jnp.where(side == 0, lower, upper)
            launch(lambda: route_copy("p", t, way, k), 0.5)

    def relay(t, way, k):
        if plan[t][way][0] == "H":
            route_copy("f", t, way, k).wait_recv()
            launch(lambda: route_copy("bf", t, way, k))
        else:
            route_copy("p", t, way, k).wait_recv()
            launch(lambda: route_copy("pair", t, way, k))

    def select(t, way, k):
        cand, sel = ref[("cand", t, way, k)], ref[("sel", t, way, k)]
        if plan[t][way][0] == "H":
            both_arrived(cand.at[0:2], ("b", t, way), k)
            sel[...] = cand[plan[t][way][3]]
        else:
            route_copy("pair", t, way, k).wait_recv()
            for n in range(2):
                sel[n] = cand[plan[t][way][3 + n]]
        launch(lambda: route_copy("l", t, way, k))

    def picked(t, way, k, place, last):
        return jnp.where(place == 4, last, ref[("cand", t, way, k)][jnp.minimum(place, 3)])

    def hand_over(t, way, k):
        route_copy("l", t, way, k).wait_recv()
        last = ref[("last", t, way, k)]
        own, other = plan[t][way][5:7]
        ref[("keep", t, way, k)][...] = picked(t, way, k, own, last[side])
        ref[("hand", t, way, k)][...] = picked(t, way, k, other, last[1 - side])
        launch(lambda: route_copy("e", t, way, k), 0.5)

    def leave(t, way, k):
        if plan[t][way][0] == "H":
            route_copy("l", t, way, k).wait_recv()
            return picked(t, way, k, plan[t][way][4], ref[("last", t, way, k)][...])
        route_copy("e", t, way, k).wait_recv()
        keep, take = ref[("keep", t, way, k)][...], ref[("take", t, way, k)][...]
        return jnp.concatenate(
            [jnp.where(side == 0, keep, take), jnp.where(side == 0, take, keep)], axis=0
        )

    def merged(t, way):
        return teams[t][0] == "F" and way == "I"

    def arrived(pieces, key):
        view = lv.at[0, 0:pieces * rows // chunks]
        pltpu.make_async_copy(view, view, ref[key + ("rcv",)].at[0]).wait()

    seen = {}

    def last_of(name, t):
        seen[(name, t)] = seen.get((name, t), 0) + 1
        return seen[(name, t)] == chunks

    def across_copy(t, way, k, g):
        piece = ref[("all", t, way, k)].at[g]
        return to_group(piece, piece, ("across", t, way), 0 if merged(t, way) else k, across)

    def mate_copy(t, way, k, g):
        piece = ref[("all", t, way, k)].at[g]
        return to_group(piece, piece, ("mate", t, way), 0 if merged(t, way) else k, mate)

    def share(t, way, k, piece):
        ref[("all", t, way, k)][grp] = piece
        launch(lambda: across_copy(t, way, k, grp))
        if (t, way) in DIRECT:
            piece = ref[("all", t, way, k)].at[grp]
            launch(lambda: to_group(piece, piece, ("mate", t, way), k, diagonal))
        launch(lambda: mate_copy(t, way, k, grp))

    def pass_on(t, way, k):
        across_copy(t, way, k, across).wait_recv()
        if (t, way) not in DIRECT:
            launch(lambda: mate_copy(t, way, k, across))

    def gathered(t, way, k):
        both_arrived(ref[("all", t, way, k)].at[0:2], ("mate", t, way), k)

    def whole(t, way, k):
        return ref[("all", t, way, k)][...].reshape(groups * rows, w)

    def dot(a, b):
        return jnp.dot(a, b, preferred_element_type=jnp.float32).astype(out_ref.dtype)

    def home_copy(t, k):
        return to_group(
            ref[("pc", t, "O", k)].at[1 - core], ref[("rcvc", t, "O", k)], ("home", t, "O"), k, mate
        )

    def back_copy(t, k):
        return to_group(
            ref[("sely", t, "O", k)], ref[("rcvy", t, "O", k)], ("back", t, "O"), k, across
        )

    def owner_side(t, k, which):
        return jnp.where(
            owner_core == core, ref[("pc", t, "O", k)][core, which], ref[("rcvc", t, "O", k)][which]
        )

    def offer(t, k, piece_of):
        for g in range(groups):
            ref[("pc", t, "O", k)][g % 2, g // 2] = piece_of(g)
        launch(lambda: home_copy(t, k), 2)

    waited = [False, False, False]

    def loaded(n):
        if not waited[n]:
            loads[n].wait()
            waited[n] = True

    def run(name, t, k):
        q = k % chunks
        slot = plan[t]["slot"]
        if name in ("I0", "G0"):
            loaded(0)
            piece = gv[plan[t]["j"], :, cols_of(q)]
            if name == "I0":
                enter(t, "I", k, piece)
            else:
                share(t, "I", k, piece)
        elif name == "I1":
            relay(t, "I", k)
        elif name == "I2":
            select(t, "I", k)
        elif name in ("IX", "OX"):
            hand_over(t, name[0], k)
        elif name == "I3":
            share(t, "I", k, leave(t, "I", k))
        elif name == "I4":
            pass_on(t, "I", k)
        elif name == "G1":
            if last_of(name, t):
                arrived(chunks, ("across", t, "I"))
                for n in range(chunks):
                    launch(lambda: mate_copy(t, "I", n, across))
        elif name == "G2":
            if last_of(name, t):
                arrived(2 * chunks, ("mate", t, "I"))
        elif name == "I5":
            loaded(1)
            gathered(t, "I", k)
            ref[("lp", t)][:, cols_of(q)] = dot(lv[slot], whole(t, "I", k))
        elif name == "R":
            loaded(2)
            product = dot(ref[("lp", t)][...], rv[slot, :, cols_of(q)])
            offer(t, k, lambda g: product[g * rows:(g + 1) * rows])
        elif name == "S0":
            n = 1 if k < chunks else 2
            loaded(n)
            table = lv if k < chunks else rv
            offer(t, k, lambda g: table[slot, g * rows:(g + 1) * rows, cols_of(q)])
        elif name == "H":
            home_copy(t, k).wait_recv()
            ref[("sely", t, "O", k)][...] = owner_side(t, k, 1 - half)
            launch(lambda: back_copy(t, k))
        elif name == "O0":
            back_copy(t, k).wait_recv()
            mine = owner_side(t, k, half)
            enter(t, "O", k, jnp.where(owner_half == half, mine, ref[("rcvy", t, "O", k)][...]))
        elif name == "O1":
            relay(t, "O", k)
        elif name == "O2":
            select(t, "O", k)
        elif name == "O3" and teams[t][0] == "F" and k < chunks:
            if last_of(name, t):
                arrived(chunks, ("l", t, "O"))
                for n in range(chunks):
                    last = ref[("last", t, "O", n)][...]
                    ref[("lrow", t)][:, cols_of(n)] = picked(t, "O", n, plan[t]["O"][4], last)
        elif name == "O3":
            piece = leave(t, "O", k)
            if teams[t][0] == "G":
                ref[("fin", t)][:, cols_of(q)] = piece
            else:
                share(t, "O", q, piece)
        elif name == "LG":
            for n in range(chunks):
                ref[("lg", t)][:, cols_of(n)] = dot(ref[("lrow", t)][...], whole(t, "I", n))
        elif name == "O4":
            pass_on(t, "O", q)
        elif name == "O5":
            gathered(t, "O", q)
            ref[("fin", t)][:, cols_of(q)] = dot(ref[("lg", t)][...], whole(t, "O", q))

    pl.semaphore_wait(barrier, 6)
    for step in timetable(teams, chunks):
        run(*step)
    for j in range(blocks):
        value = ref[("fin", 0)][...]
        for t in range(1, blocks):
            value = jnp.where(plan[t]["j"] == j, ref[("fin", t)][...], value)
        out_ref[j] = value
    for n in range(3):
        loaded(n)
    all_sent()


def per_device_fused(gradient, left_factor, right_factor, block_owner):
    blocks, rows, width = gradient.shape
    columns = lax.axis_size("fsdp")
    groups = lax.axis_size("grp")
    far, near = columns // 2, columns // 4
    sides = {"far": (far, near), "near": (near, far)}
    teams = tuple(
        (team[0],) + tuple((way[0],) + sides[way[1]] for way in team[1:]) for team in TEAMS
    )
    held = scratch_of(teams, CHUNKS, blocks, columns, groups, rows, width, gradient.dtype)
    return pl.pallas_call(
        functools.partial(
            preconditioner_kernel, teams, CHUNKS, tuple(held), columns, groups, blocks, rows, width
        ),
        out_shape=pltpu.VMEM(gradient.shape, gradient.dtype),
        in_specs=[pl.BlockSpec(memory_space=pl.ANY)] * 4,
        out_specs=pl.BlockSpec(memory_space=pltpu.VMEM),
        scratch_shapes=list(held.values()),
        compiler_params=pltpu.CompilerParams(
            collective_id=0, has_side_effects=True, vmem_limit_bytes=VMEM_LIMIT
        ),
    )(block_owner, gradient, left_factor, right_factor)


def per_device_any(gradient, left_factor, right_factor, block_owner):
    blocks = gradient.shape[0]
    columns = lax.axis_size("fsdp")
    fits = (
        blocks == left_factor.shape[0]
        and blocks == len(TEAMS)
        and lax.axis_size("grp") == 4
        and columns == 8
        and gradient.shape[2] % (CHUNKS * 128) == 0
    )
    body = per_device_fused if fits else per_device
    return body(gradient, left_factor, right_factor, block_owner)


def solution(mesh):
    return jax.shard_map(
        per_device_any,
        mesh=mesh,
        in_specs=(
            P("fsdp", "grp", None),
            P(("fsdp", "grp"), None, None),
            P(("fsdp", "grp"), None, None),
            P(),
        ),
        out_specs=P("fsdp", "grp", None),
        check_vma=False,
    )
```

```python
import functools
import math

import jax
import jax.numpy as jnp
from jax import lax
from jax.experimental import pallas as pl
from jax.experimental.pallas import tpu as pltpu
from jax.sharding import PartitionSpec as P

MESH = pl.DeviceIdType.MESH
CHUNKS = 4
COARSE = 2
SENT = 5
DIRECT = ((0, "I"),)
VMEM_LIMIT = 66519040
TEAMS = (('G', ('H', 'far'), ('H', 'near')), ('F', ('H', 'far')), ('F', ('H', 'near')))
ROUTE_STEPS = {"H": "0123", "X": "012X3"}
WHEN = {
    ('I0', 0): (0, 1, 2, 3),
    ('S0', 2): (4, 20, 23, 36, 43, 49, 58, 69),
    ('S0', 1): (5, 6, 7, 8, 9, 10, 14, 19),
    ('H', 2): (11, 26, 31, 40, 48, 53, 67, 76),
    ('H', 1): (12, 13, 15, 16, 17, 18, 22, 27),
    ('I1', 0): (21, 30, 33, 37),
    ('G0', 1): (24, 25, 28, 29),
    ('O0', 1): (32, 34, 38, 39, 41, 44, 54, 68),
    ('I2', 0): (35, 42, 47, 59),
    ('I3', 0): (45, 52, 61, 74),
    ('O0', 2): (46, 60, 70, 78, 84, 92, 97, 105),
    ('O1', 1): (50, 57, 65, 72, 81, 82, 89, 99),
    ('G1', 1): (51, 55, 64, 66),
    ('G2', 1): (56, 63, 71, 75),
    ('O1', 2): (62, 91, 94, 100, 107, 116, 120, 127),
    ('O2', 1): (73, 83, 88, 101, 106, 109, 123, 132),
    ('I4', 0): (77, 80, 96, 104),
    ('G0', 2): (79, 85, 87, 98),
    ('O2', 2): (86, 118, 128, 135, 142, 144, 150, 152),
    ('I5', 0): (90, 95, 103, 111),
    ('O3', 1): (93, 102, 108, 121, 130, 138, 139, 147),
    ('G1', 2): (110, 112, 115, 117),
    ('O3', 2): (113, 141, 149, 155, 161, 165, 170, 172),
    ('R', 0): (114, 119, 124, 129),
    ('H', 0): (122, 126, 133, 137),
    ('LG', 1): (125,),
    ('G2', 2): (131, 134, 136, 145),
    ('O0', 0): (140, 143, 148, 157),
    ('O4', 1): (146, 153, 160, 162),
    ('O1', 0): (151, 158, 163, 168),
    ('O5', 1): (154, 159, 166, 167),
    ('LG', 2): (156,),
    ('O2', 0): (164, 169, 173, 174),
    ('O4', 2): (171, 176, 179, 180),
    ('O5', 2): (175, 178, 182, 183),
    ('O3', 0): (177, 181, 184, 185),
}


def per_device(gradient, left_factor, right_factor, block_owner):
    local_blocks = gradient.shape[0]
    piece_rows = gradient.shape[1]
    block_width = gradient.shape[2]
    slot_count = left_factor.shape[0]
    columns = lax.axis_size("fsdp")
    groups = lax.axis_size("grp")
    column = lax.axis_index("fsdp")
    owners_all = block_owner.reshape(columns, local_blocks)
    dest_column = owners_all // groups
    dest_group = owners_all % groups
    mine_column = lax.dynamic_index_in_dim(dest_column, column, 0, keepdims=False)
    column_ids = jnp.arange(columns, dtype=jnp.int32)
    matching = mine_column[None, :] == column_ids[:, None]
    pick_send = matching.astype(jnp.bfloat16)
    outgoing = jnp.einsum(
        "cj,jrd->crd", pick_send, gradient, preferred_element_type=jnp.float32
    ).astype(jnp.bfloat16)
    arrived = lax.all_to_all(
        outgoing.reshape(columns * piece_rows, block_width),
        "fsdp",
        split_axis=0,
        concat_axis=0,
        tiled=True,
    )
    arrived = arrived.reshape(columns, piece_rows, block_width)
    toward = dest_column == column
    live_source = jnp.sum(toward.astype(jnp.int32), axis=1) > 0
    target = jnp.sum(jnp.where(toward, dest_group, 0), axis=1)
    same_owner = (target[None, :] == target[:, None]) & live_source[None, :] & live_source[:, None]
    before = column_ids[None, :] < column_ids[:, None]
    rank_slot = jnp.sum((same_owner & before).astype(jnp.int32), axis=1)
    group_ids = jnp.arange(groups, dtype=jnp.int32)
    slot_ids = jnp.arange(slot_count, dtype=jnp.int32)
    routing = (
        live_source[None, None, :]
        & (target[None, None, :] == group_ids[:, None, None])
        & (rank_slot[None, None, :] == slot_ids[None, :, None])
    )
    routing = routing.astype(jnp.bfloat16)
    packed = jnp.einsum(
        "oks,srd->kord", routing, arrived, preferred_element_type=jnp.float32
    ).astype(jnp.bfloat16)
    packed = packed.reshape(slot_count, groups * piece_rows, block_width)
    blocks = lax.all_to_all(packed, "grp", split_axis=1, concat_axis=1, tiled=True)
    left_product = jnp.einsum(
        "kab,kbc->kac", left_factor, blocks, preferred_element_type=jnp.float32
    ).astype(jnp.bfloat16)
    result = jnp.einsum(
        "kab,kbc->kac", left_product, right_factor, preferred_element_type=jnp.float32
    ).astype(jnp.bfloat16)
    returned = lax.all_to_all(result, "grp", split_axis=1, concat_axis=1, tiled=True)
    returned = returned.reshape(slot_count, groups, piece_rows, block_width)
    unpacked = jnp.einsum(
        "oks,kord->srd", routing, returned, preferred_element_type=jnp.float32
    ).astype(jnp.bfloat16)
    homeward = lax.all_to_all(
        unpacked.reshape(columns * piece_rows, block_width),
        "fsdp",
        split_axis=0,
        concat_axis=0,
        tiled=True,
    )
    homeward = homeward.reshape(columns, piece_rows, block_width)
    return jnp.einsum(
        "cj,crd->jrd", pick_send, homeward, preferred_element_type=jnp.float32
    ).astype(jnp.bfloat16)


def stages_of(team, chunks):
    if team[0] == "G":
        steps = [w + n for w, way in zip("IO", team[1:]) for n in ROUTE_STEPS[way[0]]]
        return [(name, chunks) for name in steps + ["I4", "I5", "R", "H"]]
    steps = ["S0", "H"] + ["O" + n for n in ROUTE_STEPS[team[1][0]]]
    found = [(name, chunks) for name in ("G0", "G1", "G2", "O4", "O5")]
    return found + [(name, 2 * chunks) for name in steps] + [("LG", 1)]


def timetable(teams, chunks):
    steps = []
    for t, team in enumerate(teams):
        for name, count in stages_of(team, chunks):
            first = chunks if name in ("O4", "O5") else 0
            for i in range(count):
                steps.append((WHEN[(name, t)][i], len(steps), name, t, first + i))
    return [step[2:] for step in sorted(steps)]


def scratch_of(teams, chunks, blocks, columns, groups, rows, width, dtype):
    w = width // chunks
    vmem = lambda *shape: pltpu.VMEM(shape, dtype)
    dma = pltpu.SemaphoreType.DMA
    held = {
        "gv": vmem(blocks, rows, width),
        "lv": vmem(blocks, width, width),
        "rv": vmem(blocks, width, width),
        "load": dma((4,)),
        "owner": pltpu.SMEM((columns * blocks,), jnp.int32),
        "sent": dma((SENT,)),
        "power": pltpu.SMEM((columns,), jnp.int32),
    }

    def copies(key, count):
        held[key + ("rcv",)] = dma((count,))

    def route(key, count, kind):
        for k in range(count):
            if kind == "H":
                held[("cand",) + key + (k,)] = vmem(4, rows, w)
                held[("last",) + key + (k,)] = vmem(rows, w)
                held[("sel",) + key + (k,)] = vmem(rows, w)
            else:
                held[("cand",) + key + (k,)] = vmem(4, rows // 2, w)
                held[("last",) + key + (k,)] = vmem(2, rows // 2, w)
                held[("sel",) + key + (k,)] = vmem(2, rows // 2, w)
                for name in ("give", "keep", "hand", "take"):
                    held[(name,) + key + (k,)] = vmem(rows // 2, w)
        for name in ("f", "b", "l") if kind == "H" else ("p", "f", "l", "e"):
            copies((name,) + key, count)
        if count > chunks:
            copies(("l",) + key, 1 + count - chunks)

    def gather(key, count, waits):
        for k in range(count):
            held[("all",) + key + (k,)] = vmem(groups, rows, w)
        for name in ("across", "mate"):
            copies((name,) + key, waits)

    def scatter(key, count):
        for k in range(count):
            held[("pc",) + key + (k,)] = vmem(2, 2, rows, w)
            held[("rcvc",) + key + (k,)] = vmem(2, rows, w)
            held[("sely",) + key + (k,)] = vmem(rows, w)
            held[("rcvy",) + key + (k,)] = vmem(rows, w)
        for name in ("home", "back"):
            copies((name,) + key, count)

    for t, team in enumerate(teams):
        held[("fin", t)] = vmem(rows, width)
        if team[0] == "G":
            route((t, "I"), chunks, team[1][0])
            gather((t, "I"), chunks, chunks)
            held[("lp", t)] = vmem(width, width)
            scatter((t, "O"), chunks)
            route((t, "O"), chunks, team[2][0])
        else:
            gather((t, "I"), chunks, 1)
            scatter((t, "O"), 2 * chunks)
            route((t, "O"), 2 * chunks, team[1][0])
            gather((t, "O"), chunks, chunks)
            held[("lrow", t)] = vmem(rows, width)
            held[("lg", t)] = vmem(rows, width)
    return held


def preconditioner_kernel(
    teams, chunks, names, columns, groups, blocks, rows, width,
    owner_hbm, g_hbm, l_hbm, r_hbm, out_ref, *rest,
):
    ref = dict(zip(names, rest))
    col = lax.axis_index("fsdp")
    grp = lax.axis_index("grp")
    core = grp % 2
    half = grp // 2
    mate = half * 2 + (1 - core)
    across = (1 - half) * 2 + core
    diagonal = (1 - half) * 2 + (1 - core)
    w = width // chunks
    zero = jnp.int32(0)

    def cols_of(q):
        return slice(q * w, (q + 1) * w)

    def partner(s):
        d, b = 0, 1
        while b < columns:
            v = (col // b) % 2
            d, b = d + b * ((1 - v) if s & b else v), 2 * b
        return d

    gv, lv, rv, owner_ref = ref["gv"], ref["lv"], ref["rv"], ref["owner"]
    loads = [
        pltpu.make_async_copy(g_hbm, gv, ref["load"].at[0]),
        pltpu.make_async_copy(l_hbm, lv, ref["load"].at[1]),
        pltpu.make_async_copy(r_hbm, rv, ref["load"].at[2]),
        pltpu.make_async_copy(owner_hbm, owner_ref, ref["load"].at[3]),
    ]
    for load in loads[::-1]:
        load.start()

    far, near = columns // 2, columns // 4
    barrier = pltpu.get_barrier_semaphore()
    for s in (1, near, far):
        pl.semaphore_signal(barrier, inc=1, device_id={"fsdp": partner(s)}, device_id_type=MESH)
    for g in (mate, across, diagonal):
        pl.semaphore_signal(barrier, inc=1, device_id={"grp": g}, device_id_type=MESH)

    def look_up(table, index):
        found = zero
        for n, value in enumerate(table):
            found = jnp.where(index == n, value, found)
        return found

    loads[3].wait()
    power = ref["power"]
    for d in range(columns):
        power[d] = jnp.int32(2 ** d)
    to = [[owner_ref[c * blocks + j] // groups for j in range(blocks)] for c in range(columns)]
    left_over = [[(jnp.int32(j), to[c][j], power[to[c][j]]) for j in range(blocks)] for c in range(columns)]
    pick, dest = [], []
    full = 2 ** columns - 1
    while len(left_over[0]) > 1:
        m = len(left_over[0])
        count = m ** columns
        tall = -(-count // 1024) * 8
        inverse = -(-(2 ** 17) // m)
        index = (
            lax.broadcasted_iota(jnp.int32, (tall, 128), 0) * 128
            + lax.broadcasted_iota(jnp.int32, (tall, 128), 1)
        )
        rest_of, reach = index, jnp.zeros((tall, 128), jnp.int32)
        for c in range(columns):
            upper = (rest_of * inverse) >> 17
            digit = rest_of - upper * m
            bit = jnp.full((tall, 128), left_over[c][m - 1][2], jnp.int32)
            for i in range(m - 1):
                bit = jnp.where(digit == i, left_over[c][i][2], bit)
            reach, rest_of = reach | bit, upper
        chosen = jnp.min(jnp.where((reach == full) & (index < count), index, count - 1))
        pick_t, dest_t = [], []
        for c in range(columns):
            upper = (chosen * inverse) >> 17
            digit, chosen = chosen - upper * m, upper
            pick_t.append(look_up([e[0] for e in left_over[c]], digit))
            dest_t.append(look_up([e[1] for e in left_over[c]], digit))
            left_over[c] = [
                tuple(jnp.where(digit <= i, b, a) for a, b in zip(left_over[c][i], left_over[c][i + 1]))
                for i in range(m - 1)
            ]
        pick.append(pick_t)
        dest.append(dest_t)
    pick.append([left_over[c][0][0] for c in range(columns)])
    dest.append([left_over[c][0][1] for c in range(columns)])

    owner_group = zero
    for c in range(columns):
        for j in range(blocks):
            owner_group = jnp.where(to[c][j] == col, owner_ref[c * blocks + j] % groups, owner_group)
    owner_core = owner_group % 2
    owner_half = owner_group // 2
    reaches = []
    for c in range(columns):
        hit = zero
        for j in range(blocks):
            hit = jnp.where(to[c][j] == col, 1, hit)
        reaches.append(hit)

    def source_of(t, d):
        found = zero
        for c in range(columns):
            found = jnp.where(dest[t][c] == d, c, found)
        return found

    def place_among(wanted, f, other):
        found = jnp.int32(other)
        for n, s in enumerate((0, 1, f, f + 1)):
            found = jnp.where(wanted == partner(s), n, found)
        return found

    side = col % 2

    def route_plan(way, origin):
        kind, f, l = way
        if kind == "H":
            return kind, f, l, place_among(origin(partner(l)), f, 0), place_among(origin(col), f, 4)
        there = partner(l) - side
        held_by = (col - side, col - side + 1, partner(f) - side, partner(f) - side + 1)

        def place(d, other):
            found, wanted = jnp.int32(other), origin(d)
            for n, c in enumerate(held_by):
                found = jnp.where(wanted == c, n, found)
            return found

        return kind, f, l, place(there, 0), place(there + 1, 0), place(col, 4), place(partner(1), 4)

    plan = []
    for t, team in enumerate(teams):
        mine = {"j": look_up(pick[t], col)}
        src = source_of(t, col)
        slot = zero
        for c in range(columns):
            slot = slot + jnp.where(c < src, reaches[c], 0)
        mine["slot"] = jnp.minimum(slot, blocks - 1)
        if team[0] == "G":
            mine["I"] = route_plan(team[1], functools.partial(source_of, t))
        mine["O"] = route_plan(team[-1], functools.partial(look_up, dest[t]))
        plan.append(mine)

    most = blocks * width // (rows // chunks)
    sent, now = [0], [0]

    def launch(copy, pieces=1):
        if max(most - n for n in sent) < pieces:
            sent.append(0)
        now[0] = next(n for n, held in enumerate(sent) if held + pieces <= most)
        copy().start()
        sent[now[0]] += pieces

    def all_sent():
        for n, pieces in enumerate(sent):
            pieces, step = (int(pieces), rows // chunks) if pieces == int(pieces) else (int(2 * pieces), rows // chunks // 2)
            over = next(b for b in range(1, blocks + 1) if pieces % b == 0 and pieces // b * step <= width)
            view = lv.at[0:over, 0:pieces // over * step]
            pltpu.make_async_copy(view, view, ref["sent"].at[n]).wait()

    def remote(src, dst, key, k, device):
        return pltpu.make_async_remote_copy(
            src_ref=src, dst_ref=dst,
            send_sem=ref["sent"].at[now[0]], recv_sem=ref[key + ("rcv",)].at[k],
            device_id=device, device_id_type=MESH,
        )

    def to_column(src, dst, key, k, s):
        return remote(src, dst, key, k, {"fsdp": partner(s)})

    def to_group(src, dst, key, k, g):
        return remote(src, dst, key, k, {"grp": g})

    def both_arrived(pair, key, k):
        pltpu.make_async_copy(pair, pair, ref[key + ("rcv",)].at[k]).wait()

    def route_copy(kind, t, way, k):
        f, l = plan[t][way][1:3]
        cand = ref[("cand", t, way, k)]
        if kind == "l":
            n = k if teams[t][0] == "G" else max(0, k - chunks + 1)
            return to_column(ref[("sel", t, way, k)], ref[("last", t, way, k)], ("l", t, way), n, l)
        if kind == "p":
            return to_column(ref[("give", t, way, k)], cand.at[side], ("p", t, way), k, 1)
        if kind == "pair":
            return to_column(cand.at[0:2], cand.at[2:4], ("f", t, way), k, f)
        if kind == "e":
            return to_column(ref[("hand", t, way, k)], ref[("take", t, way, k)], ("e", t, way), k, 1)
        if kind == "f":
            return to_column(cand.at[0], cand.at[2], ("f", t, way), k, f)
        if kind == "b":
            return to_column(cand.at[0], cand.at[1], ("b", t, way), k, 1)
        return to_column(cand.at[2], cand.at[3], ("b", t, way), k, 1)

    def enter(t, way, k, piece):
        cand = ref[("cand", t, way, k)]
        if plan[t][way][0] == "H":
            cand[0] = piece
            launch(lambda: route_copy("f", t, way, k))
            launch(lambda: route_copy("b", t, way, k))
        else:
            upper, lower = piece[: rows // 2], piece[rows // 2:]
            cand[side] = jnp.where(side == 0, upper, lower)
            ref[("give", t, way, k)][...] = jnp.where(side == 0, lower, upper)
            launch(lambda: route_copy("p", t, way, k), 0.5)

    def relay(t, way, k):
        if plan[t][way][0] == "H":
            route_copy("f", t, way, k).wait_recv()
            launch(lambda: route_copy("bf", t, way, k))
        else:
            route_copy("p", t, way, k).wait_recv()
            launch(lambda: route_copy("pair", t, way, k))

    def select(t, way, k):
        cand, sel = ref[("cand", t, way, k)], ref[("sel", t, way, k)]
        if plan[t][way][0] == "H":
            both_arrived(cand.at[0:2], ("b", t, way), k)
            sel[...] = cand[plan[t][way][3]]
        else:
            route_copy("pair", t, way, k).wait_recv()
            for n in range(2):
                sel[n] = cand[plan[t][way][3 + n]]
        launch(lambda: route_copy("l", t, way, k))

    def picked(t, way, k, place, last):
        return jnp.where(place == 4, last, ref[("cand", t, way, k)][jnp.minimum(place, 3)])

    def hand_over(t, way, k):
        route_copy("l", t, way, k).wait_recv()
        last = ref[("last", t, way, k)]
        own, other = plan[t][way][5:7]
        ref[("keep", t, way, k)][...] = picked(t, way, k, own, last[side])
        ref[("hand", t, way, k)][...] = picked(t, way, k, other, last[1 - side])
        launch(lambda: route_copy("e", t, way, k), 0.5)

    def leave(t, way, k):
        if plan[t][way][0] == "H":
            route_copy("l", t, way, k).wait_recv()
            return picked(t, way, k, plan[t][way][4], ref[("last", t, way, k)][...])
        route_copy("e", t, way, k).wait_recv()
        keep, take = ref[("keep", t, way, k)][...], ref[("take", t, way, k)][...]
        return jnp.concatenate(
            [jnp.where(side == 0, keep, take), jnp.where(side == 0, take, keep)], axis=0
        )

    def merged(t, way):
        return teams[t][0] == "F" and way == "I"

    def arrived(pieces, key):
        view = lv.at[0, 0:pieces * rows // chunks]
        pltpu.make_async_copy(view, view, ref[key + ("rcv",)].at[0]).wait()

    seen = {}

    def last_of(name, t):
        seen[(name, t)] = seen.get((name, t), 0) + 1
        return seen[(name, t)] == chunks

    def across_copy(t, way, k, g):
        piece = ref[("all", t, way, k)].at[g]
        return to_group(piece, piece, ("across", t, way), 0 if merged(t, way) else k, across)

    def mate_copy(t, way, k, g):
        piece = ref[("all", t, way, k)].at[g]
        return to_group(piece, piece, ("mate", t, way), 0 if merged(t, way) else k, mate)

    def share(t, way, k, piece):
        ref[("all", t, way, k)][grp] = piece
        launch(lambda: across_copy(t, way, k, grp))
        if (t, way) in DIRECT:
            piece = ref[("all", t, way, k)].at[grp]
            launch(lambda: to_group(piece, piece, ("mate", t, way), k, diagonal))
        launch(lambda: mate_copy(t, way, k, grp))

    def pass_on(t, way, k):
        across_copy(t, way, k, across).wait_recv()
        if (t, way) not in DIRECT:
            launch(lambda: mate_copy(t, way, k, across))

    def gathered(t, way, k):
        both_arrived(ref[("all", t, way, k)].at[0:2], ("mate", t, way), k)

    def whole(t, way, k):
        return ref[("all", t, way, k)][...].reshape(groups * rows, w)

    def dot(a, b):
        return jnp.dot(a, b, preferred_element_type=jnp.float32).astype(out_ref.dtype)

    def home_copy(t, k):
        return to_group(
            ref[("pc", t, "O", k)].at[1 - core], ref[("rcvc", t, "O", k)], ("home", t, "O"), k, mate
        )

    def back_copy(t, k):
        return to_group(
            ref[("sely", t, "O", k)], ref[("rcvy", t, "O", k)], ("back", t, "O"), k, across
        )

    def owner_side(t, k, which):
        return jnp.where(
            owner_core == core, ref[("pc", t, "O", k)][core, which], ref[("rcvc", t, "O", k)][which]
        )

    def offer(t, k, piece_of):
        for g in range(groups):
            ref[("pc", t, "O", k)][g % 2, g // 2] = piece_of(g)
        launch(lambda: home_copy(t, k), 2)

    waited = [False, False, False]

    def loaded(n):
        if not waited[n]:
            loads[n].wait()
            waited[n] = True

    def run(name, t, k):
        q = k % chunks
        slot = plan[t]["slot"]
        if name in ("I0", "G0"):
            loaded(0)
            piece = gv[plan[t]["j"], :, cols_of(q)]
            if name == "I0":
                enter(t, "I", k, piece)
            else:
                share(t, "I", k, piece)
        elif name == "I1":
            relay(t, "I", k)
        elif name == "I2":
            select(t, "I", k)
        elif name in ("IX", "OX"):
            hand_over(t, name[0], k)
        elif name == "I3":
            share(t, "I", k, leave(t, "I", k))
        elif name == "I4":
            pass_on(t, "I", k)
        elif name == "G1":
            if last_of(name, t):
                arrived(chunks, ("across", t, "I"))
                for n in range(chunks):
                    launch(lambda: mate_copy(t, "I", n, across))
        elif name == "G2":
            if last_of(name, t):
                arrived(2 * chunks, ("mate", t, "I"))
        elif name == "I5":
            loaded(1)
            gathered(t, "I", k)
            ref[("lp", t)][:, cols_of(q)] = dot(lv[slot], whole(t, "I", k))
        elif name == "R":
            loaded(2)
            product = dot(ref[("lp", t)][...], rv[slot, :, cols_of(q)])
            offer(t, k, lambda g: product[g * rows:(g + 1) * rows])
        elif name == "S0":
            n = 1 if k < chunks else 2
            loaded(n)
            table = lv if k < chunks else rv
            offer(t, k, lambda g: table[slot, g * rows:(g + 1) * rows, cols_of(q)])
        elif name == "H":
            home_copy(t, k).wait_recv()
            ref[("sely", t, "O", k)][...] = owner_side(t, k, 1 - half)
            launch(lambda: back_copy(t, k))
        elif name == "O0":
            back_copy(t, k).wait_recv()
            mine = owner_side(t, k, half)
            enter(t, "O", k, jnp.where(owner_half == half, mine, ref[("rcvy", t, "O", k)][...]))
        elif name == "O1":
            relay(t, "O", k)
        elif name == "O2":
            select(t, "O", k)
        elif name == "O3" and teams[t][0] == "F" and k < chunks:
            if last_of(name, t):
                arrived(chunks, ("l", t, "O"))
                for n in range(chunks):
                    last = ref[("last", t, "O", n)][...]
                    ref[("lrow", t)][:, cols_of(n)] = picked(t, "O", n, plan[t]["O"][4], last)
        elif name == "O3":
            piece = leave(t, "O", k)
            if teams[t][0] == "G":
                ref[("fin", t)][:, cols_of(q)] = piece
            else:
                share(t, "O", q, piece)
        elif name == "LG":
            for n in range(chunks):
                ref[("lg", t)][:, cols_of(n)] = dot(ref[("lrow", t)][...], whole(t, "I", n))
        elif name == "O4":
            pass_on(t, "O", q)
        elif name == "O5":
            gathered(t, "O", q)
            ref[("fin", t)][:, cols_of(q)] = dot(ref[("lg", t)][...], whole(t, "O", q))

    pl.semaphore_wait(barrier, 6)
    for step in timetable(teams, chunks):
        run(*step)
    for j in range(blocks):
        value = ref[("fin", 0)][...]
        for t in range(1, blocks):
            value = jnp.where(plan[t]["j"] == j, ref[("fin", t)][...], value)
        out_ref[j] = value
    for n in range(3):
        loaded(n)
    all_sent()


def per_device_fused(gradient, left_factor, right_factor, block_owner):
    blocks, rows, width = gradient.shape
    columns = lax.axis_size("fsdp")
    groups = lax.axis_size("grp")
    far, near = columns // 2, columns // 4
    sides = {"far": (far, near), "near": (near, far)}
    teams = tuple(
        (team[0],) + tuple((way[0],) + sides[way[1]] for way in team[1:]) for team in TEAMS
    )
    held = scratch_of(teams, CHUNKS, blocks, columns, groups, rows, width, gradient.dtype)
    return pl.pallas_call(
        functools.partial(
            preconditioner_kernel, teams, CHUNKS, tuple(held), columns, groups, blocks, rows, width
        ),
        out_shape=pltpu.VMEM(gradient.shape, gradient.dtype),
        in_specs=[pl.BlockSpec(memory_space=pl.ANY)] * 4,
        out_specs=pl.BlockSpec(memory_space=pltpu.VMEM),
        scratch_shapes=list(held.values()),
        compiler_params=pltpu.CompilerParams(
            collective_id=0, has_side_effects=True, vmem_limit_bytes=VMEM_LIMIT
        ),
    )(block_owner, gradient, left_factor, right_factor)


def per_device_any(gradient, left_factor, right_factor, block_owner):
    blocks = gradient.shape[0]
    columns = lax.axis_size("fsdp")
    fits = (
        blocks == left_factor.shape[0]
        and blocks == len(TEAMS)
        and lax.axis_size("grp") == 4
        and columns == 8
        and gradient.shape[2] % (CHUNKS * 128) == 0
    )
    body = per_device_fused if fits else per_device
    return body(gradient, left_factor, right_factor, block_owner)


def solution(mesh):
    return jax.shard_map(
        per_device_any,
        mesh=mesh,
        in_specs=(
            P("fsdp", "grp", None),
            P(("fsdp", "grp"), None, None),
            P(("fsdp", "grp"), None, None),
            P(),
        ),
        out_specs=P("fsdp", "grp", None),
        check_vma=False,
    )
```
